32 devices in a mesh: dp: 1 (over z), tp: 4 (over y), ep: 8 (over x, core).
Axes of the slice: x: 4, y: 4, z: 1, core: 2. Of those that a mesh axis runs over, the one named last changes fastest.
The devices are a block of a 4x4x8 slice.
Arguments:
- hidden_in: bfloat16 [8, 1024, 4096], P(('dp', 'ep'))
- expert_ids: int32 [8, 1024, 2], P(('dp', 'ep'))
- slot_ids: int32 [8, 1024, 2], P(('dp', 'ep'))
- attn_gain: bfloat16 [4096], replicated
- w_query: bfloat16 [4096, 32, 128], P(None, 'tp')
- w_key: bfloat16 [4096, 32, 128], P(None, 'tp')
- w_value: bfloat16 [4096, 32, 128], P(None, 'tp')
- w_out: bfloat16 [32, 128, 4096], P('tp')
- ffn_gain: bfloat16 [4096], replicated
- w_gate: bfloat16 [4096, 11008], P(None, 'tp')
- w_up: bfloat16 [4096, 11008], P(None, 'tp')
- w_down: bfloat16 [11008, 4096], P('tp')
- moe_gain: bfloat16 [4096], replicated
- w_router: bfloat16 [4096, 8], replicated
- exp_gate: bfloat16 [8, 4096, 1376], P('ep')
- exp_up: bfloat16 [8, 4096, 1376], P('ep')
- exp_down: bfloat16 [8, 1376, 4096], P('ep')
Outputs:
- output: bfloat16 [8, 1024, 4096], P(('dp', 'ep'))
All inputs are finite; a program needn't handle non-finite values.
Results may differ from the reference program's by a relative error of at most 0.00953262.
Values are sent between devices in bfloat16 or wider.
A program may use at most 768 MiB of HBM per device.

```python
import math
import jax
import jax.numpy as jnp
from jax import lax

D = 4096
HEADS = 32
HEAD = 128
FF = 11008
EXPERTS = 8
TOP = 2
FE = 1376
SEQ = 1024
SEQS_DEV = 1
GROUP = 8
TOK_DEV = SEQS_DEV * SEQ
TOKENS = GROUP * TOK_DEV
MEAN_LOAD = TOK_DEV * TOP // EXPERTS
CAP = 3 * MEAN_LOAD // 2
EPS = 1e-6
ROPE_BASE = 10000.0


def rms_norm(x_val, gain):
    x_f32 = x_val.astype(jnp.float32)
    inv_rms = lax.rsqrt(jnp.mean(x_f32 * x_f32, axis=-1, keepdims=True) + EPS)
    return (x_f32 * inv_rms * gain.astype(jnp.float32)).astype(jnp.bfloat16)


def rope_tables():
    inv_freq = ROPE_BASE ** (-jnp.arange(HEAD // 2, dtype=jnp.float32) * (2.0 / HEAD))
    angle = jnp.arange(SEQ, dtype=jnp.float32)[:, None] * inv_freq[None, :]
    return jnp.cos(angle), jnp.sin(angle)


def apply_rope(x_val, cos_tab, sin_tab):
    half_dim = x_val.shape[-1] // 2
    lower = x_val[..., :half_dim]
    upper = x_val[..., half_dim:]
    cos_b = cos_tab[:, None, :]
    sin_b = sin_tab[:, None, :]
    return jnp.concatenate([lower * cos_b - upper * sin_b, upper * cos_b + lower * sin_b], axis=-1)


def dense_sequence(h_seq, attn_gain, w_query, w_key, w_value, w_out, ffn_gain, w_gate, w_up, w_down):
    width = HEADS * HEAD
    cos_tab, sin_tab = rope_tables()
    x_norm = rms_norm(h_seq, attn_gain)
    q_f32 = jnp.dot(x_norm, w_query.reshape(D, width), preferred_element_type=jnp.float32).reshape(SEQ, HEADS, HEAD)
    k_f32 = jnp.dot(x_norm, w_key.reshape(D, width), preferred_element_type=jnp.float32).reshape(SEQ, HEADS, HEAD)
    query = apply_rope(q_f32, cos_tab, sin_tab).astype(jnp.bfloat16)
    key_proj = apply_rope(k_f32, cos_tab, sin_tab).astype(jnp.bfloat16)
    value_proj = jnp.dot(x_norm, w_value.reshape(D, width), preferred_element_type=jnp.float32).astype(jnp.bfloat16).reshape(SEQ, HEADS, HEAD)
    scores = jnp.einsum('qhe,khe->hqk', query.astype(jnp.float32), key_proj.astype(jnp.float32)) * HEAD ** -0.5
    causal = jnp.arange(SEQ)[:, None] >= jnp.arange(SEQ)[None, :]
    attn_prob = jax.nn.softmax(jnp.where(causal[None], scores, -1e30), axis=-1).astype(jnp.bfloat16)
    context = jnp.einsum('hqk,khe->qhe', attn_prob.astype(jnp.float32), value_proj.astype(jnp.float32)).astype(jnp.bfloat16)
    attn_out = jnp.dot(context.reshape(SEQ, width), w_out.reshape(width, D), preferred_element_type=jnp.float32)
    after_attn = (h_seq.astype(jnp.float32) + attn_out).astype(jnp.bfloat16)
    f_norm = rms_norm(after_attn, ffn_gain)
    gate_pre = jnp.dot(f_norm, w_gate, preferred_element_type=jnp.float32)
    up_pre = jnp.dot(f_norm, w_up, preferred_element_type=jnp.float32)
    hidden_act = (jax.nn.silu(gate_pre) * up_pre).astype(jnp.bfloat16)
    ffn_out = jnp.dot(hidden_act, w_down, preferred_element_type=jnp.float32)
    return after_attn.astype(jnp.float32) + ffn_out


def source_routing(key):
    key_shift, key_label, key_token = jax.random.split(key, 3)
    shift = jax.random.randint(key_shift, (EXPERTS // 2,), 0, MEAN_LOAD // 2 + 1)
    shift = shift.at[0].set(MEAN_LOAD // 2)
    paired = jnp.stack([MEAN_LOAD + shift, MEAN_LOAD - shift], axis=1).reshape(EXPERTS)
    counts = paired[jax.random.permutation(key_label, EXPERTS)]
    ends = jnp.cumsum(counts)
    starts = ends - counts
    position = jnp.arange(TOK_DEV * TOP, dtype=jnp.int32)
    owner = jnp.sum((position[:, None] >= ends[None, :]).astype(jnp.int32), axis=1)
    slot_row = position - starts[owner]
    column = jax.random.permutation(key_token, TOK_DEV)
    expert_col = owner.reshape(TOP, TOK_DEV)[:, column].T
    slot_col = slot_row.reshape(TOP, TOK_DEV)[:, column].T
    return expert_col.astype(jnp.int32), slot_col.astype(jnp.int32)


def draw_routing(key):
    expert_all, slot_all = lax.map(source_routing, jax.random.split(key, GROUP))
    out_shape = (GROUP * SEQS_DEV, SEQ, TOP)
    return expert_all.reshape(out_shape), slot_all.reshape(out_shape)


def normal_weight(key, shape, scale):
    return (jax.random.normal(key, shape, jnp.float32) * scale).astype(jnp.bfloat16)


def gain_vector(key):
    return (1.0 + 0.3 * jax.random.normal(key, (D,), jnp.float32)).astype(jnp.bfloat16)


def setup_inputs(seed: int = 0, part: int = 0) -> dict:
    root = jax.random.key(seed)
    part_key = jax.random.fold_in(root, part)
    key_hidden, key_route = jax.random.split(part_key, 2)
    weight_keys = jax.random.split(root, 14)
    width = HEADS * HEAD
    query_scale = math.sqrt(math.log(SEQ) / 2.0) * D ** -0.5
    expert_ids, slot_ids = draw_routing(key_route)
    return {
        'hidden_in': normal_weight(key_hidden, (GROUP * SEQS_DEV, SEQ, D), 1.0),
        'expert_ids': expert_ids,
        'slot_ids': slot_ids,
        'attn_gain': gain_vector(weight_keys[0]),
        'w_query': normal_weight(weight_keys[1], (D, HEADS, HEAD), query_scale),
        'w_key': normal_weight(weight_keys[2], (D, HEADS, HEAD), D ** -0.5),
        'w_value': normal_weight(weight_keys[3], (D, HEADS, HEAD), D ** -0.5),
        'w_out': normal_weight(weight_keys[4], (HEADS, HEAD, D), 2.0 * width ** -0.5),
        'ffn_gain': gain_vector(weight_keys[5]),
        'w_gate': normal_weight(weight_keys[6], (D, FF), D ** -0.5),
        'w_up': normal_weight(weight_keys[7], (D, FF), D ** -0.5),
        'w_down': normal_weight(weight_keys[8], (FF, D), FF ** -0.5),
        'moe_gain': gain_vector(weight_keys[9]),
        'w_router': normal_weight(weight_keys[10], (D, EXPERTS), 2.0 * D ** -0.5),
        'exp_gate': normal_weight(weight_keys[11], (EXPERTS, D, FE), D ** -0.5),
        'exp_up': normal_weight(weight_keys[12], (EXPERTS, D, FE), D ** -0.5),
        'exp_down': normal_weight(weight_keys[13], (EXPERTS, FE, D), 2.0 * FE ** -0.5),
    }


def reference(hidden_in, expert_ids, slot_ids, attn_gain, w_query, w_key, w_value, w_out, ffn_gain, w_gate, w_up, w_down, moe_gain, w_router, exp_gate, exp_up, exp_down):
    tokens = hidden_in.reshape(TOKENS, D)
    route_ids = expert_ids.reshape(TOKENS, TOP)
    slots = slot_ids.reshape(TOKENS, TOP)
    u_norm = rms_norm(tokens, moe_gain)
    logits = jnp.dot(u_norm, w_router, preferred_element_type=jnp.float32)
    gates = jax.nn.softmax(jnp.take_along_axis(logits, route_ids, axis=1), axis=-1)
    token_of = jnp.broadcast_to(jnp.arange(TOKENS, dtype=jnp.int32)[:, None], (TOKENS, TOP))
    flat_pos = (((token_of // TOK_DEV) * EXPERTS + route_ids) * CAP + slots).reshape(-1)
    row_token = jnp.full((GROUP * EXPERTS * CAP,), TOKENS, jnp.int32).at[flat_pos].set(token_of.reshape(-1))
    row_gate = jnp.zeros((GROUP * EXPERTS * CAP,), jnp.float32).at[flat_pos].set(gates.reshape(-1))
    row_token = row_token.reshape(GROUP, EXPERTS, CAP).transpose(1, 0, 2).reshape(EXPERTS, GROUP * CAP)
    row_gate = row_gate.reshape(GROUP, EXPERTS, CAP).transpose(1, 0, 2).reshape(EXPERTS, GROUP * CAP)

    def expert_step(moe_acc, slab):
        rows, gate_rows, w_one, w_three, w_two = slab
        x_rows = jnp.take(u_norm, rows, axis=0, mode='fill', fill_value=0)
        gate_pre = jnp.dot(x_rows, w_one, preferred_element_type=jnp.float32)
        up_pre = jnp.dot(x_rows, w_three, preferred_element_type=jnp.float32)
        hidden_act = (jax.nn.silu(gate_pre) * up_pre).astype(jnp.bfloat16)
        expert_out = jnp.dot(hidden_act, w_two, preferred_element_type=jnp.float32).astype(jnp.bfloat16)
        return moe_acc.at[rows].add(gate_rows[:, None] * expert_out.astype(jnp.float32), mode='drop'), None

    moe_sum = lax.scan(expert_step, jnp.zeros((TOKENS, D), jnp.float32), (row_token, row_gate, exp_gate, exp_up, exp_down))[0]
    dense_out = lax.map(lambda h_seq: dense_sequence(h_seq, attn_gain, w_query, w_key, w_value, w_out, ffn_gain, w_gate, w_up, w_down), hidden_in)
    return (dense_out.reshape(TOKENS, D) + moe_sum).reshape(GROUP * SEQS_DEV, SEQ, D).astype(jnp.bfloat16)
```

```python
import functools

import jax
import jax.numpy as jnp
from jax import lax
from jax.experimental import pallas as pl
from jax.experimental.pallas import tpu as pltpu
from jax.sharding import PartitionSpec as P

EPS = 1e-6
ROPE_BASE = 10000.0
QBLK = 256
MESH = pl.DeviceIdType.MESH
F32, BF16 = jnp.float32, jnp.bfloat16


def rope_tables(seq_len, head_dim):
    inv_freq = ROPE_BASE ** (-jnp.arange(head_dim // 2, dtype=F32) * (2.0 / head_dim))
    angle = jnp.arange(seq_len, dtype=F32)[:, None] * inv_freq[None, :]
    cos, sin = jnp.cos(angle), jnp.sin(angle)
    return jnp.concatenate([cos, cos], axis=1), jnp.concatenate([-sin, sin], axis=1)


def attn_kernel(scale, cos_ref, sin_ref, q_ref, k_ref, v_ref, o_ref, kr_ref):
    half = q_ref.shape[2] // 2
    q_rows = q_ref.shape[1]

    def rope(val, cos, sin):
        return (val * cos + pltpu.roll(val, half, 1) * sin).astype(BF16)

    kr_ref[...] = rope(k_ref[0], cos_ref[...], sin_ref[...])
    for blk in range(q_rows // QBLK):
        base = blk * QBLK
        rows = pl.ds(base, QBLK)
        query = rope(q_ref[0, rows, :], cos_ref[rows, :], sin_ref[rows, :])

        def score(lo, hi):
            return lax.dot_general(query, kr_ref[lo:hi, :], (((1,), (1,)), ((), ())), preferred_element_type=F32)

        diag = score(base, base + QBLK)
        row = lax.broadcasted_iota(jnp.int32, diag.shape, 0)
        col = lax.broadcasted_iota(jnp.int32, diag.shape, 1)
        scores = jnp.where(row >= col, diag, -1e30)
        if blk:
            scores = jnp.concatenate([score(0, base), scores], axis=1)
        top = jnp.max(scores, axis=1, keepdims=True)
        prob = jnp.exp((scores - top) * scale)
        prob = (prob * (1.0 / jnp.sum(prob, axis=1, keepdims=True))).astype(BF16)
        o_ref[rows, :] = jnp.dot(prob, v_ref[0, :base + QBLK, :], preferred_element_type=F32).astype(BF16)


def attention(query, keys, values, cos, sin):
    heads, rows, head_dim = query.shape
    tab = pl.BlockSpec((rows, head_dim), lambda h: (0, 0))
    spec = pl.BlockSpec((1, rows, head_dim), lambda h: (h, 0, 0))
    return pl.pallas_call(
        functools.partial(attn_kernel, head_dim ** -0.5),
        grid=(heads,),
        in_specs=[tab, tab, spec, spec, spec],
        out_specs=pl.BlockSpec((rows, head_dim), lambda h: (0, h)),
        out_shape=jax.ShapeDtypeStruct((rows, heads * head_dim), BF16),
        scratch_shapes=[pltpu.VMEM((rows, head_dim), BF16)],
        cost_estimate=pl.CostEstimate(flops=16 * heads * rows * rows * head_dim, bytes_accessed=heads * head_dim * rows * 12, transcendentals=heads * rows * rows),
    )(cos, sin, query, keys, values)


TILE = 256
CHUNKS = 4
NT_SLOTS = 3
NN_SLOTS = 4


def layer_kernel(tp, ep, ctx, w_out, x, gain, wg, wu, wd, recv, eg, eu, ed, row_of, gates,
                 out, c_l, c_r, c_o, a_l, a_r, a_o, wx, back,
                 lhs, h, fbuf, r1, r2, ybuf, a_own, a_in, a_mine, out_q, sel, wb1, wb2, wb3,
                 send_sem, recv_sem, ysend, yrecv, wsend, wrecv, sem1, sem2, sem3, lsem, osem):
    seq, d_model = out.shape
    rows = seq // CHUNKS
    quarter = rows // tp
    width = d_model // tp
    slots_all = recv.shape[0]
    sub = slots_all // ep
    me = lax.axis_index('tp')
    my_e = lax.axis_index('ep')
    right, left, far = lax.rem(me + 1, tp), lax.rem(me + tp - 1, tp), lax.rem(me + 2, tp)

    barrier = pltpu.get_barrier_semaphore()
    for peer in (right, far, left):
        pl.semaphore_signal(barrier, inc=1, device_id={'tp': peer}, device_id_type=MESH)
    for k in range(1, ep):
        pl.semaphore_signal(barrier, inc=1, device_id={'ep': lax.rem(my_e + k, ep)}, device_id_type=MESH)
    pl.semaphore_wait(barrier, 3 + ep - 1)

    def at(start, size, align):
        return pl.ds(pl.multiple_of(start, align), size)

    def remote(kind, c, d, src, dst):
        return pltpu.make_async_remote_copy(
            src_ref=src, dst_ref=dst, send_sem=send_sem.at[kind, c, d], recv_sem=recv_sem.at[kind, c, d],
            device_id={'tp': (right, left)[d]}, device_id_type=MESH)

    half = rows // 2

    def c_first(c, d):
        piece = at(c * rows, rows, rows)
        return remote(0, c, d, ctx.at[piece, :], (c_l, c_r)[d].at[piece, :])

    def c_second(c, d):
        piece = at(c * rows + d * half, half, half)
        return remote(1, c, d, (c_l, c_r)[d].at[piece, :], c_o.at[piece, :])

    def a_first(c, d):
        piece = at(c * rows, rows, rows)
        return remote(2, c, d, a_own.at[piece, :], (a_l, a_r)[d].at[piece, :])

    def a_second(c, d):
        piece = at(c * rows + d * half, half, half)
        return remote(3, c, d, (a_l, a_r)[d].at[piece, :], a_o.at[piece, :])

    q_half = quarter // 2

    def r_first(c, d):
        return remote(4, c, d, fbuf.at[lax.rem(c, 2), at(far * quarter + d * q_half, q_half, q_half), :], r1.at[c, d])

    def r_second(c, d):
        return remote(5, c, d, fbuf.at[lax.rem(c, 2), at((right, left)[d] * quarter, quarter, quarter), :], r2.at[c, d])

    def o_first(c, d):
        return remote(6, c, d, out_q.at[c], out.at[at(c * rows + me * quarter, quarter, quarter), :])

    def o_second(c, d):
        piece = at(c * rows + (left, right)[d] * quarter + d * q_half, q_half, q_half)
        return remote(7, c, d, out.at[piece, :], out.at[piece, :])

    def start(make, c):
        make(c, 0).start()
        make(c, 1).start()

    def arrived(make, c):
        make(c, 0).wait_recv()
        make(c, 1).wait_recv()

    def sent(make, c):
        make(c, 0).wait_send()
        make(c, 1).wait_send()

    share = w_out.shape[0] // ep
    cores = 2
    chips = ep // cores

    def w_first(k):
        peer = lax.rem(me + k, tp)
        return pltpu.make_async_remote_copy(
            src_ref=w_out.at[at(my_e * share, share, share), at(peer * width, width, width)],
            dst_ref=wx.at[me, at(my_e * share, share, share), :],
            send_sem=wsend.at[0, 0, k], recv_sem=wrecv.at[0, 0, k], device_id={'tp': peer}, device_id_type=MESH)

    def w_piece(stage, m, k, owner, peer):
        piece = wx.at[lax.rem(me + tp - k, tp), at(owner * share, share, share), :]
        return pltpu.make_async_remote_copy(
            src_ref=piece, dst_ref=piece, send_sem=wsend.at[stage, m, k], recv_sem=wrecv.at[stage, m, k],
            device_id={'ep': peer}, device_id_type=MESH)

    def w_second(m, k):
        return w_piece(1, m, k, my_e, lax.rem(my_e + cores * m, ep))

    def w_third(m, k):
        return w_piece(2, m, k, lax.rem(my_e + ep - cores * m, ep), my_e + 1 - 2 * lax.rem(my_e, 2))

    def each(count, low, do):
        def outer(m, carry):
            def inner(k, carry):
                do(m, k)
                return carry
            return lax.fori_loop(1, tp, inner, carry)
        lax.fori_loop(low, count, outer, 0)

    def w_start():
        lax.fori_loop(1, tp, lambda k, carry: (w_first(k).start(), carry)[1], 0)

    def w_spread():
        lax.fori_loop(1, tp, lambda k, carry: (w_first(k).wait_recv(), carry)[1], 0)
        each(chips, 1, lambda m, k: w_second(m, k).start())
        each(1, 0, lambda m, k: w_third(m, k).start())

    def w_pair():
        def pass_on(m, k):
            w_second(m, k).wait_recv()
            w_third(m, k).start()
        each(chips, 1, pass_on)

    def w_done():
        each(chips, 0, lambda m, k: w_third(m, k).wait_recv())

    def w_sent():
        lax.fori_loop(1, tp, lambda k, carry: (w_first(k).wait_send(), carry)[1], 0)
        each(chips, 1, lambda m, k: w_second(m, k).wait_send())
        each(chips, 0, lambda m, k: w_third(m, k).wait_send())

    def gate_up(wa, wb, mid=None):
        total = wa.shape[0]
        full, tail = total // TILE, total % TILE

        def copies(i, slot, n):
            return [pltpu.make_async_copy(w.at[at(i * TILE, n, 32), :], wb1.at[slot, k, pl.ds(0, n), :], sem1.at[slot, k]) for k, w in enumerate((wa, wb))]

        def go(i, slot, n=TILE):
            for cp in copies(i, slot, n):
                cp.start()

        def ready(i, slot, n=TILE):
            for cp in copies(i, slot, n):
                cp.wait()

        def product(slot, n):
            dims = (((1,), (1,)), ((), ()))
            gate = lax.dot_general(lhs[...], wb1[slot, 0, :n, :], dims, preferred_element_type=F32)
            up = lax.dot_general(lhs[...], wb1[slot, 1, :n, :], dims, preferred_element_type=F32)
            return (jax.nn.silu(gate) * up).astype(BF16)

        ahead = NT_SLOTS - 1
        for j in range(ahead):
            go(j, j)

        def step(i, carry):
            nxt = i + ahead
            pl.when(nxt < full)(lambda: go(nxt, lax.rem(nxt, NT_SLOTS)))
            if tail:
                pl.when(nxt == full)(lambda: go(full, full % NT_SLOTS, tail))
            slot = lax.rem(i, NT_SLOTS)
            ready(i, slot)
            h[:, at(i * TILE, TILE, TILE)] = product(slot, TILE)
            if mid is not None:
                pl.when(i == full // 2)(mid)
            return carry

        lax.fori_loop(0, full, step, 0)
        if tail:
            ready(full, full % NT_SLOTS, tail)
            h[:, full * TILE:full * TILE + tail] = product(full % NT_SLOTS, tail)

    def columns(left_ref, depth, tiles, fetch, use):
        ahead = NN_SLOTS - 1

        def go(i, slot):
            for cp in fetch(i, slot):
                cp.start()

        for j in range(ahead):
            go(j, j)

        def step(i, carry):
            nxt = i + ahead
            pl.when(nxt < tiles)(lambda: go(nxt, lax.rem(nxt, NN_SLOTS)))
            slot = lax.rem(i, NN_SLOTS)
            for cp in fetch(i, slot):
                cp.wait()
            use(i, slot, jnp.dot(left_ref[:, :depth], wb2[slot, :depth, :], preferred_element_type=F32))
            return carry

        lax.fori_loop(0, tiles, step, 0)

    def whole_depth(w):
        def fetch(i, slot):
            return [pltpu.make_async_copy(w.at[:, at(i * TILE, TILE, TILE)], wb2.at[slot, pl.ds(0, w.shape[0]), :], sem2.at[slot, 0])]
        return fetch

    def set_off(c, carry):
        start(c_first, c)
        return carry

    def c_forward(c, carry):
        arrived(c_first, c)
        start(c_second, c)
        return carry

    def y_copy(e):
        return pltpu.make_async_remote_copy(
            src_ref=ybuf.at[pl.ds(e * sub, sub), :], dst_ref=back.at[at(my_e * sub, sub, sub), :],
            send_sem=ysend.at[e], recv_sem=yrecv.at[my_e], device_id={'ep': e}, device_id_type=MESH)

    def y_arrival(e):
        return pltpu.make_async_remote_copy(
            src_ref=ybuf.at[pl.ds(e * sub, sub), :], dst_ref=back.at[pl.ds(e * sub, sub), :],
            send_sem=ysend.at[e], recv_sem=yrecv.at[e], device_id={'ep': e}, device_id_type=MESH)

    def y_local(e):
        return pltpu.make_async_copy(ybuf.at[pl.ds(e * sub, sub), :], back.at[pl.ds(e * sub, sub), :], ysend.at[e])

    def expert(r, carry):
        load = pltpu.make_async_copy(recv.at[at(r * TILE, TILE, TILE), :], lhs, lsem.at[0])
        load.start()
        load.wait()
        gate_up(eg, eu)

        def keep(i, slot, acc):
            ybuf[at(r * TILE, TILE, TILE), at(i * TILE, TILE, TILE)] = acc.astype(BF16)
        columns(h, ed.shape[0], d_model // TILE, whole_depth(ed), keep)
        pl.when(r == 0)(w_spread)
        return carry
    w_start()
    lax.fori_loop(0, CHUNKS, set_off, 0)
    lax.fori_loop(0, slots_all // TILE, expert, 0)
    for e in range(ep):
        pl.when(e != my_e)(lambda e=e: y_copy(e).start())
        pl.when(e == my_e)(lambda e=e: y_local(e).start())
    w_pair()
    lax.fori_loop(0, CHUNKS, c_forward, 0)

    def project(c, carry):
        arrived(c_second, c)
        piece = at(c * rows, rows, rows)
        loads = [pltpu.make_async_copy(src.at[piece, :], lhs.at[:, at(who * width, width, width)], lsem.at[k])
                 for k, (src, who) in enumerate(((ctx, me), (c_r, right), (c_o, far), (c_l, left)))]
        loads.append(pltpu.make_async_copy(x.at[piece, at(me * width, width, width)], a_own.at[piece, :], lsem.at[4]))
        for cp in loads:
            cp.start()
        for cp in loads:
            cp.wait()

        def keep(i, slot, acc):
            block = (piece, at(i * TILE, TILE, TILE))
            a_own[block] = (a_own[block].astype(F32) + acc).astype(BF16)

        def fetch(i, slot):
            cols = at(i * TILE, TILE, TILE)
            own = pltpu.make_async_copy(w_out.at[:, at(me * width + i * TILE, TILE, TILE)], wb2.at[slot, at(me * width, width, width), :], sem2.at[slot, 0])
            rest = [pltpu.make_async_copy(wx.at[who, :, cols], wb2.at[slot, at(who * width, width, width), :], sem2.at[slot, k])
                    for k, who in ((1, right), (2, far), (3, left))]
            return [own] + rest
        pl.when(c == 0)(w_done)
        columns(lhs, d_model, width // TILE, fetch, keep)
        start(a_first, c)

        def forward():
            arrived(a_first, c - 1)
            start(a_second, c - 1)
        pl.when((c >= 1) & (c < CHUNKS - 1))(forward)
        return carry
    lax.fori_loop(0, CHUNKS, project, 0)

    def a_forward(c):
        arrived(a_first, c)
        start(a_second, c)

    def reduce_on(c):
        for d, who in ((0, right), (1, left)):
            r_first(c, d).wait_recv()

            def add(k, carry, d=d, who=who):
                block = (lax.rem(c, 2), at(who * quarter + d * q_half + k * 8, 8, 8), slice(None))
                fbuf[block] = fbuf[block] + r1[c, d, at(k * 8, 8, 8), :]
                return carry
            lax.fori_loop(0, q_half // 8, add, 0)
            r_second(c, d).start()

    def o_local(c):
        return pltpu.make_async_copy(out_q.at[c], out.at[at(c * rows + me * quarter, quarter, quarter), :], osem.at[c])

    def finish(c):
        arrived(r_second, c)

        def add(k, carry):
            part = at(k * 16, 16, 16)
            total = fbuf[lax.rem(c, 2), at(me * quarter + k * 16, 16, 16), :] + (r2[c, 0, part, :] + r2[c, 1, part, :])
            out_q[c, part, :] = (a_mine[c, part, :].astype(F32) + total).astype(BF16)
            return carry
        lax.fori_loop(0, quarter // 16, add, 0)
        start(o_first, c)
        o_local(c).start()

    def o_forward(c):
        arrived(o_first, c)
        start(o_second, c)

    def y_back():
        for e in range(ep):
            pl.when(e != my_e)(lambda e=e: y_arrival(e).wait_recv())
            pl.when(e == my_e)(lambda e=e: y_local(e).wait())

    def ffn(c, carry):
        arrived(a_second, c)
        piece = at(c * rows, rows, rows)
        loads = [pltpu.make_async_copy(src.at[piece, :], a_in.at[k], lsem.at[k]) for k, src in enumerate((a_r, a_o, a_l))]
        for cp in loads:
            cp.start()
        for cp in loads:
            cp.wait()
        parts = ((None, me), (0, right), (1, far), (2, left))

        def norm(k, carry):
            block = at(k * 16, 16, 16)
            vals = [(a_own[at(c * rows + k * 16, 16, 16), :] if p is None else a_in[p, block, :]).astype(F32) for p, _ in parts]
            square = sum(jnp.sum(v * v, axis=1, keepdims=True) for v in vals)
            inv = lax.rsqrt(square / d_model + EPS)
            for v, (_, who) in zip(vals, parts):
                cols = at(who * width, width, width)
                lhs[block, cols] = (v * inv * gain[:, cols]).astype(BF16)
            return carry
        lax.fori_loop(0, rows // 16, norm, 0)
        for p, who in parts:
            mine = at(me * quarter, quarter, quarter)
            val = a_own[at(c * rows + me * quarter, quarter, quarter), :] if p is None else a_in[p, mine, :]
            a_mine[c, :, at(who * width, width, width)] = val
        for j in range(row_of.shape[1]):
            target = row_of[piece, j:j + 1]
            sel[j * rows:(j + 1) * rows, :] = jnp.where(lax.broadcasted_iota(jnp.int32, (rows, slots_all), 1) == target, 1.0, 0.0).astype(BF16)

        def mid():
            pl.when(c == 0)(lambda: a_forward(CHUNKS - 2))
            pl.when(c >= 1)(lambda: reduce_on(c - 1))
        gate_up(wg, wu, mid)
        @pl.when(c == 0)
        def _():
            a_forward(CHUNKS - 1)
            y_back()

        @pl.when(c >= 2)
        def _():
            o_forward(c - 2)
            sent(r_first, c - 2)
            sent(r_second, c - 2)

        def keep(i, slot, acc):
            copies = jnp.dot(sel[...], wb3[slot], preferred_element_type=F32)
            for j in range(row_of.shape[1]):
                acc = acc + gates[piece, j:j + 1] * copies[j * rows:(j + 1) * rows]
            fbuf[lax.rem(c, 2), :, at(i * TILE, TILE, TILE)] = acc
        down = whole_depth(wd)

        def fetch(i, slot):
            return down(i, slot) + [pltpu.make_async_copy(back.at[:, at(i * TILE, TILE, TILE)], wb3.at[slot], sem3.at[slot])]
        columns(h, wd.shape[0], d_model // TILE, fetch, keep)
        start(r_first, c)
        pl.when(c >= 1)(lambda: finish(c - 1))
        return carry
    lax.fori_loop(0, CHUNKS, ffn, 0)
    reduce_on(CHUNKS - 1)
    o_forward(CHUNKS - 2)
    finish(CHUNKS - 1)
    o_forward(CHUNKS - 1)

    def drain(c, carry):
        arrived(o_second, c)
        o_local(c).wait()
        for make in (c_first, c_second, a_first, a_second, o_first, o_second):
            sent(make, c)

        @pl.when(c >= CHUNKS - 2)
        def _():
            sent(r_first, c)
            sent(r_second, c)
        return carry
    lax.fori_loop(0, CHUNKS, drain, 0)
    for e in range(ep):
        pl.when(e != my_e)(lambda e=e: y_copy(e).wait_send())
    w_sent()


def fused_layer(tp, ep, ctx, w_out, x, gain, wg, wu, wd, recv, eg, eu, ed, row_of, gates):
    seq, d_model = x.shape
    rows = seq // CHUNKS
    quarter = rows // tp
    width = d_model // tp
    hidden = wd.shape[0]
    slots_all = recv.shape[0]
    top_k = row_of.shape[1]
    any_spec = pl.BlockSpec(memory_space=pl.ANY)
    vmem_spec = pl.BlockSpec(memory_space=pltpu.VMEM)
    part = jax.ShapeDtypeStruct((seq, width), BF16)
    outs = pl.pallas_call(
        functools.partial(layer_kernel, tp, ep),
        out_shape=[jax.ShapeDtypeStruct((seq, d_model), BF16)] + [part] * 6 + [jax.ShapeDtypeStruct((tp, w_out.shape[0], width), BF16), jax.ShapeDtypeStruct((slots_all, d_model), BF16)],
        in_specs=[any_spec] * 3 + [vmem_spec] + [any_spec] * 7 + [vmem_spec] * 2,
        out_specs=[any_spec] * 9,
        scratch_shapes=[
            pltpu.VMEM((rows, d_model), BF16),
            pltpu.VMEM((rows, hidden), BF16),
            pltpu.VMEM((2, rows, d_model), F32),
            pltpu.VMEM((CHUNKS, 2, quarter // 2, d_model), F32),
            pltpu.VMEM((CHUNKS, 2, quarter, d_model), F32),
            pltpu.VMEM((slots_all, d_model), BF16),
            pltpu.VMEM((seq, width), BF16),
            pltpu.VMEM((3, rows, width), BF16),
            pltpu.VMEM((CHUNKS, quarter, d_model), BF16),
            pltpu.VMEM((CHUNKS, quarter, d_model), BF16),
            pltpu.VMEM((top_k * rows, slots_all), BF16),
            pltpu.VMEM((NT_SLOTS, 2, TILE, d_model), BF16),
            pltpu.VMEM((NN_SLOTS, d_model, TILE), BF16),
            pltpu.VMEM((NN_SLOTS, slots_all, TILE), BF16),
            pltpu.SemaphoreType.DMA((8, CHUNKS, 2)),
            pltpu.SemaphoreType.DMA((8, CHUNKS, 2)),
            pltpu.SemaphoreType.DMA((ep,)),
            pltpu.SemaphoreType.DMA((ep,)),
            pltpu.SemaphoreType.DMA((3, ep // 2, tp)),
            pltpu.SemaphoreType.DMA((3, ep // 2, tp)),
            pltpu.SemaphoreType.DMA((NT_SLOTS, 2)),
            pltpu.SemaphoreType.DMA((NN_SLOTS, 4)),
            pltpu.SemaphoreType.DMA((NN_SLOTS,)),
            pltpu.SemaphoreType.DMA((5,)),
            pltpu.SemaphoreType.DMA((CHUNKS,)),
        ],
        compiler_params=pltpu.CompilerParams(collective_id=0, has_side_effects=True, vmem_limit_bytes=67043328),
        cost_estimate=pl.CostEstimate(flops=6 * seq * d_model * hidden, bytes_accessed=300 * 2 ** 20, transcendentals=seq * hidden),
    )(ctx, w_out, x, gain, wg, wu, wd, recv, eg, eu, ed, row_of, gates)
    return outs[0]


def solution(mesh):
    tok_spec = P(('dp', 'ep'), None, None)
    col_spec = P(None, 'tp', None)
    exp_spec = P('ep', None, None)
    in_specs = (tok_spec, tok_spec, tok_spec, P(None), col_spec, col_spec, col_spec, P('tp', None, None), P(None), P(None, 'tp'), P(None, 'tp'), P('tp', None), P(None), P(None, None), exp_spec, exp_spec, exp_spec)
    tp = mesh.shape['tp']
    ep = mesh.shape['ep']

    def layer_local(hidden_in, expert_ids, slot_ids, attn_gain, w_query, w_key, w_value, w_out, ffn_gain, w_gate, w_up, w_down, moe_gain, w_router, exp_gate, exp_up, exp_down):
        _, seq, d_model = hidden_in.shape
        heads, head_dim = w_query.shape[1:]
        experts = w_router.shape[1]
        top_k = expert_ids.shape[2]
        cap = 3 * seq * top_k // (2 * experts)
        sub = cap // tp
        rank = lax.axis_index('tp')
        x = hidden_in[0]
        x_f32 = x.astype(F32)
        unit = x_f32 * lax.rsqrt(jnp.mean(x_f32 * x_f32, axis=-1, keepdims=True) + EPS)
        n = (unit * attn_gain.astype(F32)).astype(BF16)
        u = (unit * moe_gain.astype(F32)).astype(BF16)

        ids, slots = expert_ids[0], slot_ids[0]
        row_of = jnp.where(slots % tp == rank, ids * sub + slots // tp, -1)
        rows = lax.broadcasted_iota(jnp.int32, (experts * sub, seq), 0)
        pick = sum((rows == row_of[:, j][None, :]) for j in range(top_k)).astype(BF16)
        send = jnp.dot(pick, u, preferred_element_type=F32).astype(BF16).reshape(experts, sub, d_model)
        recv = lax.all_to_all(send, 'ep', 0, 0, tiled=True).reshape(experts * sub, d_model)
        logits = jnp.dot(u, w_router, preferred_element_type=F32)
        picked = [jnp.sum(jnp.where(lax.broadcasted_iota(jnp.int32, logits.shape, 1) == ids[:, j:j + 1], logits, 0.0), axis=1, keepdims=True) for j in range(top_k)]
        gates = jax.nn.softmax(jnp.concatenate(picked, axis=1), axis=-1)

        n, _ = lax.optimization_barrier((n, send))
        cos, sin = rope_tables(seq, head_dim)
        q = jnp.einsum('sd,dhe->hse', n, w_query, preferred_element_type=F32)
        k = jnp.einsum('sd,dhe->hse', n, w_key, preferred_element_type=F32)
        v = jnp.einsum('sd,dhe->hse', n, w_value, preferred_element_type=F32).astype(BF16)
        ctx = attention(q, k, v, cos, sin)
        out = fused_layer(tp, ep, ctx, w_out.reshape(heads * head_dim, d_model), x, ffn_gain.astype(F32)[None], w_gate.T, w_up.T, w_down, recv,
                          exp_gate[0].T, exp_up[0].T, exp_down[0], row_of, gates)
        return out[None]

    return jax.shard_map(layer_local, mesh=mesh, in_specs=in_specs, out_specs=tok_spec, check_vma=False)
```

```python
import functools

import jax
import jax.numpy as jnp
import numpy as np
from jax import lax
from jax.experimental import pallas as pl
from jax.experimental.pallas import tpu as pltpu
from jax.sharding import PartitionSpec as P

EPS = 1e-6
ROPE_BASE = 10000.0
LOG2E = 1.4426950408889634
MESH = pl.DeviceIdType.MESH
F32, BF16 = jnp.float32, jnp.bfloat16


def rope_tables(seq_len, head_dim):
    inv_freq = np.float32(ROPE_BASE) ** (-np.arange(head_dim // 2, dtype=np.float32) * np.float32(2.0 / head_dim))
    angle = np.arange(seq_len, dtype=np.float32)[:, None] * inv_freq[None, :]
    cos, sin = np.cos(angle), np.sin(angle)
    return np.concatenate([cos, cos], axis=1), np.concatenate([-sin, sin], axis=1)


def prep_kernel(tp, blocks, x_ref, gain_ref, wr_ref, ids_ref, slots_ref, n_ref, route_ref, send_ref, u_ref, pick_ref):
    step = pl.program_id(0)
    size, cols = x_ref.shape[0], send_ref.shape[1]
    top_k = ids_ref.shape[0]
    slots_all = send_ref.shape[0]
    sub = slots_all // wr_ref.shape[0]

    @pl.when(step < blocks)
    def _():
        x = x_ref[...].astype(F32)
        unit = x * lax.rsqrt(jnp.mean(x * x, axis=-1, keepdims=True) + EPS)
        n_ref[...] = (unit * gain_ref[0:1, :]).astype(BF16)
        u = (unit * gain_ref[1:2, :]).astype(BF16)
        mine = pl.ds(pl.multiple_of(step * size, size), size)
        u_ref[mine, :] = u
        logits = lax.dot_general(wr_ref[...], u, (((1,), (1,)), ((), ())), preferred_element_type=F32)
        expert = lax.broadcasted_iota(jnp.int32, logits.shape, 0)
        picked = [jnp.sum(jnp.where(expert == ids_ref[j:j + 1, mine], logits, 0.0), axis=0, keepdims=True) for j in range(top_k)]
        top = functools.reduce(jnp.maximum, picked)
        weights = [jnp.exp(p - top) for p in picked]
        total = sum(weights)
        for j in range(top_k):
            route_ref[top_k + j:top_k + j + 1, mine] = weights[j] / total

    @pl.when(step == blocks)
    def _():
        rank = lax.axis_index('tp')
        rows = lax.broadcasted_iota(jnp.int32, pick_ref.shape, 0)
        hit = None
        for j in range(top_k):
            slot = slots_ref[j:j + 1, :]
            row_of = jnp.where(lax.rem(slot, tp) == rank, ids_ref[j:j + 1, :] * sub + lax.div(slot, tp), -1)
            route_ref[j:j + 1, :] = row_of.astype(F32)
            match = rows == row_of
            hit = match if hit is None else hit | match
        pick_ref[...] = jnp.where(hit, 1.0, 0.0).astype(BF16)

    @pl.when(step >= blocks)
    def _():
        part = pl.ds(pl.multiple_of((step - blocks) * cols, cols), cols)
        send_ref[...] = jnp.dot(pick_ref[...], u_ref[:, part], preferred_element_type=F32).astype(BF16)


def prepare(tp, x, gains, router, ids, slots, slots_all):
    seq, d_model = x.shape
    size, cols = 256, 512
    blocks, parts = seq // size, d_model // cols
    token = lambda i: (jnp.minimum(i, blocks - 1), 0)
    fixed = lambda i: (0, 0)
    return pl.pallas_call(
        functools.partial(prep_kernel, tp, blocks),
        grid=(blocks + parts,),
        in_specs=[pl.BlockSpec((size, d_model), token), pl.BlockSpec(gains.shape, fixed), pl.BlockSpec(router.shape, fixed),
                  pl.BlockSpec(ids.shape, fixed), pl.BlockSpec(slots.shape, fixed)],
        out_specs=[pl.BlockSpec((size, d_model), token), pl.BlockSpec((8, seq), fixed),
                   pl.BlockSpec((slots_all, cols), lambda i: (0, jnp.maximum(i - blocks, 0)))],
        out_shape=[jax.ShapeDtypeStruct((seq, d_model), BF16), jax.ShapeDtypeStruct((8, seq), F32), jax.ShapeDtypeStruct((slots_all, d_model), BF16)],
        scratch_shapes=[pltpu.VMEM((seq, d_model), BF16), pltpu.VMEM((slots_all, seq), BF16)],
        cost_estimate=pl.CostEstimate(flops=2 * slots_all * seq * d_model, bytes_accessed=6 * seq * d_model, transcendentals=0),
    )(x, gains, router, ids, slots)


def relay_kernel(heads, *refs):
    sources, o_ref = refs[:-1], refs[-1]
    depth, head_dim = o_ref.shape[0], sources[0].shape[1]
    block = 256
    span = block // heads
    row = lax.broadcasted_iota(jnp.int32, (block, block), 0)
    col = lax.broadcasted_iota(jnp.int32, (block, block), 1)
    order = jnp.where(col == (row % span) * heads + row // span, 1.0, 0.0).astype(BF16)
    for g in range(depth // span):
        for w, ref in enumerate(sources):
            moved = jnp.dot(order, ref[g * block:(g + 1) * block, :], preferred_element_type=F32).astype(BF16)
            for k in range(heads):
                lane = (w * heads + k) * head_dim
                o_ref[g * span:(g + 1) * span, lane:lane + head_dim] = moved[k * span:(k + 1) * span]


TILE = 256
CHUNKS = 4
PAIRS = 2
E_BLOCKS = 2
NT_SLOTS = 3
NN_SLOTS = 4


def layer_kernel(tp, ep, heads, top_k, n, wq, wk, wv, w_out, x, gain, wg, wu, wd, send, eg, eu, ed, route, cos_ref, sin_ref,
                 out, wqkv, c_l, c_r, c_o, a_l, a_r, a_o, wx, recv, y, back,
                 r1, r2, a_own, a_mine, out_q, wb1, wb2, wb3,
                 send_sem, recv_sem, dsend, drecv, ysend, yrecv, ysem, wsend, wrecv, sem1, sem2, sem3, lsem, osem):
    seq, d_model = out.shape
    rows = seq // CHUNKS
    quarter = rows // tp
    width = d_model // tp
    slots_all = recv.shape[0]
    sub = slots_all // ep
    me = lax.axis_index('tp')
    my_e = lax.axis_index('ep')
    right, left, far = lax.rem(me + 1, tp), lax.rem(me + tp - 1, tp), lax.rem(me + 2, tp)

    barrier = pltpu.get_barrier_semaphore()
    for peer in (right, far, left):
        pl.semaphore_signal(barrier, inc=1, device_id={'tp': peer}, device_id_type=MESH)
    for k in range(1, ep):
        pl.semaphore_signal(barrier, inc=1, device_id={'ep': lax.rem(my_e + k, ep)}, device_id_type=MESH)
    pl.semaphore_wait(barrier, 3 + ep - 1)

    def at(start, size, align):
        return pl.ds(pl.multiple_of(start, align), size)

    held = {}

    def remote(kind, c, d, src, dst):
        return pltpu.make_async_remote_copy(
            src_ref=src, dst_ref=dst, send_sem=send_sem.at[kind, c, d], recv_sem=recv_sem.at[kind, c, d],
            device_id={'tp': (right, left)[d]}, device_id_type=MESH)

    half = rows // 2

    def c_first(c, d):
        piece = at(c * rows, rows, rows)
        return remote(0, c, d, held['qkv'].at[piece, pl.ds(0, width)], (c_l, c_r)[d].at[piece, :])

    def c_second(c, d):
        piece = at(c * rows + d * half, half, half)
        return remote(1, c, d, (c_l, c_r)[d].at[piece, :], c_o.at[piece, :])

    def a_first(c, d):
        piece = at(c * rows, rows, rows)
        return remote(2, c, d, a_own.at[piece, :], (a_l, a_r)[d].at[piece, :])

    def a_second(c, d):
        piece = at(c * rows + d * half, half, half)
        return remote(3, c, d, (a_l, a_r)[d].at[piece, :], a_o.at[piece, :])

    q_half = quarter // 2

    def r_first(c, d):
        return remote(4, c, d, held['fbuf'].at[lax.rem(c, 2), at(far * quarter + d * q_half, q_half, q_half), :], r1.at[lax.rem(c, 2), d])

    def r_second(c, d):
        return remote(5, c, d, held['fbuf'].at[lax.rem(c, 2), at((right, left)[d] * quarter, quarter, quarter), :], r2.at[lax.rem(c, 2), d])

    def o_first(c, d):
        return remote(6, c, d, out_q.at[c], out.at[at(c * rows + me * quarter, quarter, quarter), :])

    def o_second(c, d):
        piece = at(c * rows + (left, right)[d] * quarter + d * q_half, q_half, q_half)
        return remote(7, c, d, out.at[piece, :], out.at[piece, :])

    def start(make, c):
        make(c, 0).start()
        make(c, 1).start()

    def arrived(make, c):
        make(c, 0).wait_recv()
        make(c, 1).wait_recv()

    def sent(make, c):
        make(c, 0).wait_send()
        make(c, 1).wait_send()

    share = w_out.shape[0] // 2
    core = lax.rem(my_e, 2)
    core_rows = at(core * share, share, share)

    def w_first(k):
        peer = lax.rem(me + k, tp)
        return pltpu.make_async_remote_copy(
            src_ref=w_out.at[core_rows, at(peer * width, width, width)], dst_ref=wx.at[me, core_rows, :],
            send_sem=wsend.at[0, k], recv_sem=wrecv.at[0, k], device_id={'tp': peer}, device_id_type=MESH)

    def w_second(k):
        piece = wx.at[lax.rem(me + tp - k, tp), core_rows, :]
        return pltpu.make_async_remote_copy(
            src_ref=piece, dst_ref=piece, send_sem=wsend.at[1, k], recv_sem=wrecv.at[1, k],
            device_id={'ep': my_e + 1 - 2 * core}, device_id_type=MESH)

    def w_start():
        for k in range(1, tp):
            w_first(k).start()

    def w_pair():
        for k in range(1, tp):
            w_first(k).wait_recv()
            w_second(k).start()

    def w_done():
        for k in range(1, tp):
            w_second(k).wait_recv()

    def w_sent():
        for k in range(1, tp):
            w_first(k).wait_send()
            w_second(k).wait_send()

    class Pair:
        def __init__(self, wa, wb):
            self.refs = (wa, wb)
            self.full, self.tail = wa.shape[0] // TILE, wa.shape[0] % TILE
            self.tiles = self.full + (self.tail > 0)

        def copies(self, i, slot, n=TILE):
            return [pltpu.make_async_copy(w.at[at(i * TILE, n, 32), :], wb1.at[slot, k, pl.ds(0, n), :], sem1.at[slot, k]) for k, w in enumerate(self.refs)]

        def go(self, i, slot, n=TILE):
            for cp in self.copies(i, slot, n):
                cp.start()

        def ready(self, i, slot, n=TILE):
            for cp in self.copies(i, slot, n):
                cp.wait()

    nt_ahead = NT_SLOTS - 1

    def gate_up(lhs, h, pair, base, then, mid=None):
        full, tail = pair.full, pair.tail

        def product(slot, n):
            dims = (((1,), (1,)), ((), ()))
            gate = lax.dot_general(lhs[:h.shape[0], :], wb1[slot, 0, :n, :], dims, preferred_element_type=F32)
            up = lax.dot_general(lhs[:h.shape[0], :], wb1[slot, 1, :n, :], dims, preferred_element_type=F32)
            return (jax.nn.silu(gate) * up).astype(BF16)

        def step(i, carry):
            nxt = i + nt_ahead
            ahead = lax.rem(base + nxt, NT_SLOTS)
            pl.when(nxt < full)(lambda: pair.go(nxt, ahead))
            if tail:
                pl.when(nxt == full)(lambda: pair.go(full, ahead, tail))
            pl.when(nxt >= pair.tiles)(lambda: then(nxt - pair.tiles, ahead))
            slot = lax.rem(base + i, NT_SLOTS)
            pair.ready(i, slot)
            h[:, at(i * TILE, TILE, TILE)] = product(slot, TILE)
            if mid is not None:
                pl.when(i == full // 2)(mid)
            return carry

        lax.fori_loop(0, full, step, 0)
        if tail:
            then(full + nt_ahead - pair.tiles, lax.rem(base + full + nt_ahead, NT_SLOTS))
            slot = lax.rem(base + full, NT_SLOTS)
            pair.ready(full, slot, tail)
            h[:, full * TILE:full * TILE + tail] = product(slot, tail)

    nn_ahead = NN_SLOTS - 1

    def go(fetch, i, slot):
        for cp in fetch(i, slot):
            cp.start()

    def prime(fetch):
        for j in range(nn_ahead):
            go(fetch, j, j)

    def columns(left_ref, m, depth, tiles, fetch, use, then=None):
        def step(i, carry):
            nxt = i + nn_ahead
            ahead = lax.rem(nxt, NN_SLOTS)
            pl.when(nxt < tiles)(lambda: go(fetch, nxt, ahead))
            if then is not None:
                pl.when(nxt >= tiles)(lambda: then(nxt - tiles, ahead))
            slot = lax.rem(i, NN_SLOTS)
            for cp in fetch(i, slot):
                cp.wait()
            use(i, slot, jnp.dot(left_ref[:m, :depth], wb2[slot, :depth, :], preferred_element_type=F32))
            return carry

        lax.fori_loop(0, tiles, step, 0)

    def whole_depth(w):
        def fetch(i, slot):
            return [pltpu.make_async_copy(w.at[:, at(i * TILE, TILE, TILE)], wb2.at[slot, pl.ds(0, w.shape[0]), :], sem2.at[slot, 0])]
        return fetch

    experts_in = Pair(eg, eu)
    ffn_in = Pair(wg, wu)
    from_qkv, from_ed, from_wd = whole_depth(wqkv), whole_depth(ed), whole_depth(wd)

    def from_out(i, slot):
        cols = at(i * TILE, TILE, TILE)
        own = pltpu.make_async_copy(w_out.at[:, at(me * width + i * TILE, TILE, TILE)], wb2.at[slot, at(me * width, width, width), :], sem2.at[slot, 0])
        rest = [pltpu.make_async_copy(wx.at[who, :, cols], wb2.at[slot, at(who * width, width, width), :], sem2.at[slot, k])
                for k, who in ((1, right), (2, far), (3, left))]
        return [own] + rest

    pair_rows = seq // PAIRS
    e_rows = slots_all // E_BLOCKS

    def c_forward(c):
        arrived(c_first, c)
        start(c_second, c)

    def d_copy(k):
        peer = lax.rem(my_e + k, ep)
        return pltpu.make_async_remote_copy(
            src_ref=send.at[at(peer * sub, sub, sub), :], dst_ref=recv.at[pl.ds((ep - k) * sub, sub), :],
            send_sem=dsend.at[k], recv_sem=drecv.at[k], device_id={'ep': peer}, device_id_type=MESH)

    own_rows = at(my_e * sub, sub, sub)
    d_local = pltpu.make_async_copy(send.at[own_rows, :], recv.at[pl.ds(0, sub), :], dsend.at[0])

    def y_copy(k):
        return pltpu.make_async_remote_copy(
            src_ref=y.at[pl.ds(k * sub, sub), :], dst_ref=back.at[own_rows, :],
            send_sem=ysend.at[k], recv_sem=yrecv.at[k], device_id={'ep': lax.rem(my_e + k, ep)}, device_id_type=MESH)

    y_local = pltpu.make_async_copy(y.at[pl.ds(0, sub), :], back.at[own_rows, :], ysend.at[0])

    def y_back():
        for k in range(1, ep):
            y_copy(k).wait_recv()
        y_local.wait()

    def a_forward(c):
        arrived(a_first, c)
        start(a_second, c)

    w_start()
    for k in range(1, ep):
        d_copy(k).start()
    d_local.start()

    head_dim = width // heads
    low = head_dim // 2

    def first_half(lhs, he, qkv, ystage):
        held['qkv'] = qkv

        def n_load(p):
            return pltpu.make_async_copy(n.at[pl.ds(p * pair_rows, pair_rows), :], lhs.at[pl.ds(0, pair_rows), :], lsem.at[0])

        def project_in(p, between=None):
            piece = pl.ds(p * pair_rows, pair_rows)
            n_load(p).wait()

            def rotate(val):
                parts = []
                for k in range(TILE // head_dim):
                    one = val[:, k * head_dim:(k + 1) * head_dim]
                    parts.append(one * cos_ref[piece, :] + pltpu.roll(one, low, 1) * sin_ref[piece, :])
                return jnp.concatenate(parts, axis=1)

            def keep(i, slot, acc):
                acc = jnp.where(i < 2 * width // TILE, rotate(acc), acc)
                qkv[piece, at(i * TILE, TILE, TILE)] = acc.astype(BF16)
            follow = from_qkv if p < PAIRS - 1 else from_out

            def then(i, slot):
                if between is not None:
                    pl.when(i == 0)(between)
                go(follow, i, slot)
            columns(lhs, pair_rows, d_model, 3 * width // TILE, from_qkv, keep, then)
            if p < PAIRS - 1:
                n_load(p + 1).start()

        def attend(c):
            base = c * rows
            keys = base + rows
            dims = (((1,), (1,)), ((), ()))

            def two(g, carry):
                for k in range(2):
                    hh = 2 * g + k
                    lane = lambda off: at(off + hh * head_dim, head_dim, head_dim)
                    query = qkv[base:keys, lane(0)]
                    scores = lax.dot_general(query, qkv[base:keys, lane(width)], dims, preferred_element_type=F32)
                    row = lax.broadcasted_iota(jnp.int32, scores.shape, 0)
                    col = lax.broadcasted_iota(jnp.int32, scores.shape, 1)
                    scores = jnp.where(row >= col, scores, -1e30)
                    if c:
                        before = lax.dot_general(query, qkv[0:base, lane(width)], dims, preferred_element_type=F32)
                        scores = jnp.concatenate([before, scores], axis=1)
                    top = jnp.max(scores, axis=1, keepdims=True)
                    prob = jnp.exp2((scores - top) * (head_dim ** -0.5 * LOG2E))
                    prob = (prob * (1.0 / jnp.sum(prob, axis=1, keepdims=True))).astype(BF16)
                    qkv[base:keys, lane(0)] = jnp.dot(prob, qkv[0:keys, lane(2 * width)], preferred_element_type=F32).astype(BF16)
                return carry
            lax.fori_loop(0, heads // 2, two, 0)

        def x_load(b):
            return pltpu.make_async_copy(recv.at[pl.ds(b * e_rows, e_rows), :], lhs.at[pl.ds(0, e_rows), :], lsem.at[0])

        def expert(b, mid):
            x_load(b).start()
            x_load(b).wait()
            last = b == E_BLOCKS - 1
            gate_up(lhs, he, experts_in, b * experts_in.tiles, ffn_in.go if last else experts_in.go, mid)
            tiles = d_model // TILE

            def put(i):
                k = lax.rem(i, 2)
                return pltpu.make_async_copy(ystage.at[k], y.at[pl.ds(b * e_rows, e_rows), at(i * TILE, TILE, TILE)], ysem.at[k])

            def keep(i, slot, acc):
                pl.when(i >= 2)(lambda: put(i - 2).wait())
                ystage[lax.rem(i, 2)] = acc.astype(BF16)
                put(i).start()
            follow = from_out if last else from_ed
            columns(he, e_rows, ed.shape[0], tiles, from_ed, keep, lambda i, slot: go(follow, i, slot))
            put(tiles - 2).wait()
            put(tiles - 1).wait()
            span = ep // E_BLOCKS
            for k in range(b * span, (b + 1) * span):
                (y_copy(k) if k else y_local).start()

        def project_out(p):
            for k in range(CHUNKS // PAIRS):
                arrived(c_second, p * (CHUNKS // PAIRS) + k)
            piece = pl.ds(p * pair_rows, pair_rows)
            here = pl.ds(0, pair_rows)
            loads = [pltpu.make_async_copy(src.at[piece, :], lhs.at[here, at(who * width, width, width)], lsem.at[k])
                     for k, (src, who) in enumerate(((c_r, right), (c_o, far), (c_l, left)))]
            loads.append(pltpu.make_async_copy(x.at[piece, at(me * width, width, width)], a_own.at[piece, :], lsem.at[4]))
            for cp in loads:
                cp.start()
            lhs[here, at(me * width, width, width)] = qkv[piece, 0:width]
            for cp in loads:
                cp.wait()

            def keep(i, slot, acc):
                block = (piece, at(i * TILE, TILE, TILE))
                a_own[block] = (a_own[block].astype(F32) + acc).astype(BF16)
            follow = from_ed if p < PAIRS - 1 else from_wd
            columns(lhs, pair_rows, d_model, width // TILE, from_out, keep, lambda i, slot: go(follow, i, slot))

        n_load(0).start()
        depth_block = 256
        pltpu.emit_pipeline(
            functools.partial(relay_kernel, heads),
            grid=(d_model // depth_block,),
            in_specs=[pl.BlockSpec((depth_block * heads, head_dim), lambda i: (i, 0))] * 3,
            out_specs=[pl.BlockSpec((depth_block, 3 * width), lambda i: (i, 0))],
        )(wq, wk, wv, wqkv)
        prime(from_qkv)
        project_in(0)
        for k in range(nt_ahead):
            experts_in.go(k, k)
        attend(0)
        start(c_first, 0)
        attend(1)
        start(c_first, 1)
        w_pair()
        project_in(1, w_done)
        c_forward(0)
        attend(2)
        c_forward(1)
        start(c_first, 2)
        attend(3)
        start(c_first, 3)
        project_out(0)
        start(a_first, 0)
        for k in range(1, ep):
            d_copy(k).wait_recv()
        d_local.wait()
        expert(0, lambda: c_forward(2))

        def late():
            a_forward(0)
            start(a_first, 1)
        c_forward(3)
        expert(1, late)
        project_out(1)
        for c in range(CHUNKS):
            sent(c_first, c)

    pl.run_scoped(
        first_half, pltpu.VMEM((max(pair_rows, e_rows), d_model), BF16), pltpu.VMEM((e_rows, ed.shape[0]), BF16),
        pltpu.VMEM((seq, 3 * width), BF16), pltpu.VMEM((2, e_rows, TILE), BF16))
    start(a_first, 2)

    def second_half(lhs, h, fbuf, a_in, sel, gates):
        held['fbuf'] = fbuf

        def reduce_on(c):
            for d, who in ((0, right), (1, left)):
                r_first(c, d).wait_recv()

                def add(k, carry, d=d, who=who):
                    block = (lax.rem(c, 2), at(who * quarter + d * q_half + k * 8, 8, 8), slice(None))
                    fbuf[block] = fbuf[block] + r1[lax.rem(c, 2), d, at(k * 8, 8, 8), :]
                    return carry
                lax.fori_loop(0, q_half // 8, add, 0)
            start(r_second, c)

        def o_local(c):
            return pltpu.make_async_copy(out_q.at[c], out.at[at(c * rows + me * quarter, quarter, quarter), :], osem.at[c])

        def finish(c):
            arrived(r_second, c)

            def add(k, carry):
                part = at(k * 16, 16, 16)
                total = fbuf[lax.rem(c, 2), at(me * quarter + k * 16, 16, 16), :] + (r2[lax.rem(c, 2), 0, part, :] + r2[lax.rem(c, 2), 1, part, :])
                out_q[c, part, :] = (a_mine[c, part, :].astype(F32) + total).astype(BF16)
                return carry
            lax.fori_loop(0, quarter // 16, add, 0)
            start(o_first, c)
            o_local(c).start()

        def o_forward(c):
            arrived(o_first, c)
            start(o_second, c)

        def from_back(i, slot):
            return pltpu.make_async_copy(back.at[:, at(i * TILE, TILE, TILE)], wb3.at[slot], sem3.at[slot])

        def copies_prime():
            for k in range(nn_ahead):
                from_back(k, k).start()

        def combine(c):
            tiles = d_model // TILE

            def step(i, carry):
                nxt = i + nn_ahead
                pl.when(nxt < tiles)(lambda: from_back(nxt, lax.rem(nxt, NN_SLOTS)).start())
                slot = lax.rem(i, NN_SLOTS)
                from_back(i, slot).wait()
                copies = jnp.dot(sel[...], wb3[slot], preferred_element_type=F32)
                block = (lax.rem(c, 2), slice(None), at(i * TILE, TILE, TILE))
                total = fbuf[block]
                for j in range(top_k):
                    total = total + gates[:, j:j + 1] * copies[j * rows:(j + 1) * rows]
                fbuf[block] = total
                return carry
            lax.fori_loop(0, tiles, step, 0)

        def ffn(c, carry):
            arrived(a_second, c)
            piece = at(c * rows, rows, rows)
            loads = [pltpu.make_async_copy(src.at[piece, :], a_in.at[k], lsem.at[k]) for k, src in enumerate((a_r, a_o, a_l))]
            for cp in loads:
                cp.start()
            for cp in loads:
                cp.wait()
            parts = ((None, me), (0, right), (1, far), (2, left))

            def norm(k, carry):
                block = at(k * 16, 16, 16)
                vals = [(a_own[at(c * rows + k * 16, 16, 16), :] if p is None else a_in[p, block, :]).astype(F32) for p, _ in parts]
                square = sum(jnp.sum(v * v, axis=1, keepdims=True) for v in vals)
                inv = lax.rsqrt(square / d_model + EPS)
                for v, (_, who) in zip(vals, parts):
                    cols = at(who * width, width, width)
                    lhs[block, cols] = (v * inv * gain[2:3, cols]).astype(BF16)
                return carry
            lax.fori_loop(0, rows // 16, norm, 0)
            for p, who in parts:
                mine = at(me * quarter, quarter, quarter)
                val = a_own[at(c * rows + me * quarter, quarter, quarter), :] if p is None else a_in[p, mine, :]
                a_mine[c, :, at(who * width, width, width)] = val
            table = jnp.transpose(route[:, piece])
            lane = lax.broadcasted_iota(jnp.int32, (rows, slots_all), 1).astype(F32)
            for j in range(top_k):
                sel[j * rows:(j + 1) * rows, :] = jnp.where(lane == table[:, j:j + 1], 1.0, 0.0).astype(BF16)
                gates[:, j:j + 1] = table[:, top_k + j:top_k + j + 1]

            def mid():
                @pl.when(c == 0)
                def _():
                    a_forward(1)
                    start(a_first, 3)
                pl.when(c >= 1)(lambda: reduce_on(c - 1))
            def after(i, slot):
                pl.when(c < CHUNKS - 1)(lambda: ffn_in.go(i, slot))
            gate_up(lhs, h, ffn_in, E_BLOCKS * experts_in.tiles + c * ffn_in.tiles, after, mid)
            pl.when(c == 0)(lambda: a_forward(2))

            @pl.when(c >= 2)
            def _():
                o_forward(c - 2)
                sent(r_first, c - 2)
                sent(r_second, c - 2)

            def keep(i, slot, acc):
                fbuf[lax.rem(c, 2), :, at(i * TILE, TILE, TILE)] = acc

            def then(i, slot):
                pl.when(c < CHUNKS - 1)(lambda: go(from_wd, i, slot))
            pl.when(c > 0)(copies_prime)
            columns(h, rows, wd.shape[0], d_model // TILE, from_wd, keep, then)

            @pl.when(c == 0)
            def _():
                a_forward(3)
                y_back()
                copies_prime()
            combine(c)
            start(r_first, c)
            pl.when(c >= 1)(lambda: finish(c - 1))
            return carry
        lax.fori_loop(0, CHUNKS, ffn, 0)
        reduce_on(CHUNKS - 1)
        o_forward(CHUNKS - 2)
        finish(CHUNKS - 1)
        o_forward(CHUNKS - 1)

        def drain(c, carry):
            arrived(o_second, c)
            o_local(c).wait()
            for make in (c_second, a_first, a_second, o_first, o_second):
                sent(make, c)

            @pl.when(c >= CHUNKS - 2)
            def _():
                sent(r_first, c)
                sent(r_second, c)
            return carry
        lax.fori_loop(0, CHUNKS, drain, 0)
        for k in range(1, ep):
            d_copy(k).wait_send()
            y_copy(k).wait_send()
        w_sent()

    pl.run_scoped(
        second_half, pltpu.VMEM((rows, d_model), BF16), pltpu.VMEM((rows, wd.shape[0]), BF16), pltpu.VMEM((2, rows, d_model), F32),
        pltpu.VMEM((3, rows, width), BF16), pltpu.VMEM((top_k * rows, slots_all), BF16), pltpu.VMEM((rows, top_k), F32))


def fused_layer(tp, ep, heads, top_k, n, wq, wk, wv, w_out, x, gains, wg, wu, wd, send, eg, eu, ed, route, cos, sin):
    seq, d_model = x.shape
    rows = seq // CHUNKS
    quarter = rows // tp
    width = d_model // tp
    hidden = wd.shape[0]
    slots_all = send.shape[0]
    any_spec = pl.BlockSpec(memory_space=pl.ANY)
    vmem_spec = pl.BlockSpec(memory_space=pltpu.VMEM)
    part = jax.ShapeDtypeStruct((seq, width), BF16)
    copies = jax.ShapeDtypeStruct((slots_all, d_model), BF16)
    outs = pl.pallas_call(
        functools.partial(layer_kernel, tp, ep, heads, top_k),
        out_shape=[jax.ShapeDtypeStruct((seq, d_model), BF16), jax.ShapeDtypeStruct((d_model, 3 * width), BF16)] + [part] * 6
        + [jax.ShapeDtypeStruct((tp, w_out.shape[0], width), BF16)] + [copies] * 3,
        in_specs=[any_spec] * 6 + [vmem_spec] + [any_spec] * 7 + [vmem_spec] * 3,
        out_specs=[any_spec] * 12,
        scratch_shapes=[
            pltpu.VMEM((2, 2, quarter // 2, d_model), F32),
            pltpu.VMEM((2, 2, quarter, d_model), F32),
            pltpu.VMEM((seq, width), BF16),
            pltpu.VMEM((CHUNKS, quarter, d_model), BF16),
            pltpu.VMEM((CHUNKS, quarter, d_model), BF16),
            pltpu.VMEM((NT_SLOTS, 2, TILE, d_model), BF16),
            pltpu.VMEM((NN_SLOTS, d_model, TILE), BF16),
            pltpu.VMEM((NN_SLOTS, slots_all, TILE), BF16),
            pltpu.SemaphoreType.DMA((8, CHUNKS, 2)),
            pltpu.SemaphoreType.DMA((8, CHUNKS, 2)),
            pltpu.SemaphoreType.DMA((ep,)),
            pltpu.SemaphoreType.DMA((ep,)),
            pltpu.SemaphoreType.DMA((ep,)),
            pltpu.SemaphoreType.DMA((ep,)),
            pltpu.SemaphoreType.DMA((2,)),
            pltpu.SemaphoreType.DMA((2, tp)),
            pltpu.SemaphoreType.DMA((2, tp)),
            pltpu.SemaphoreType.DMA((NT_SLOTS, 2)),
            pltpu.SemaphoreType.DMA((NN_SLOTS, 4)),
            pltpu.SemaphoreType.DMA((NN_SLOTS,)),
            pltpu.SemaphoreType.DMA((5,)),
            pltpu.SemaphoreType.DMA((CHUNKS,)),
        ],
        compiler_params=pltpu.CompilerParams(collective_id=0, has_side_effects=True, vmem_limit_bytes=67043328),
        cost_estimate=pl.CostEstimate(flops=6 * seq * d_model * hidden, bytes_accessed=300 * 2 ** 20, transcendentals=seq * hidden),
    )(n, wq, wk, wv, w_out, x, gains, wg, wu, wd, send, eg, eu, ed, route, cos, sin)
    return outs[0]


def solution(mesh):
    tok_spec = P(('dp', 'ep'), None, None)
    col_spec = P(None, 'tp', None)
    exp_spec = P('ep', None, None)
    in_specs = (tok_spec, tok_spec, tok_spec, P(None), col_spec, col_spec, col_spec, P('tp', None, None), P(None), P(None, 'tp'), P(None, 'tp'), P('tp', None), P(None), P(None, None), exp_spec, exp_spec, exp_spec)
    tp = mesh.shape['tp']
    ep = mesh.shape['ep']

    def layer_local(hidden_in, expert_ids, slot_ids, attn_gain, w_query, w_key, w_value, w_out, ffn_gain, w_gate, w_up, w_down, moe_gain, w_router, exp_gate, exp_up, exp_down):
        _, seq, d_model = hidden_in.shape
        heads, head_dim = w_query.shape[1:]
        experts = w_router.shape[1]
        top_k = expert_ids.shape[2]
        cap = 3 * seq * top_k // (2 * experts)
        sub = cap // tp
        x = hidden_in[0]
        gains = jnp.stack([attn_gain, moe_gain, ffn_gain]).astype(F32)
        n, route, send = prepare(tp, x, gains, w_router.T, expert_ids[0].T, slot_ids[0].T, experts * sub)
        cos, sin = rope_tables(seq, head_dim)
        flat = lambda w: w.reshape(d_model * heads, head_dim)
        out = fused_layer(tp, ep, heads, top_k, n, flat(w_query), flat(w_key), flat(w_value), w_out.reshape(heads * head_dim, d_model), x,
                          gains, w_gate.T, w_up.T, w_down, send,
                          exp_gate[0].T, exp_up[0].T, exp_down[0], route, cos, sin)
        return out[None]

    return jax.shard_map(layer_local, mesh=mesh, in_specs=in_specs, out_specs=tok_spec, check_vma=False)
```

```python
import functools

import jax
import jax.numpy as jnp
import numpy as np
from jax import lax
from jax.experimental import pallas as pl
from jax.experimental.pallas import tpu as pltpu
from jax.sharding import PartitionSpec as P

EPS = 1e-6
ROPE_BASE = 10000.0
LOG2E = 1.4426950408889634
MESH = pl.DeviceIdType.MESH
F32, BF16 = jnp.float32, jnp.bfloat16


def rope_tables(seq_len, head_dim):
    inv_freq = np.float32(ROPE_BASE) ** (-np.arange(head_dim // 2, dtype=np.float32) * np.float32(2.0 / head_dim))
    angle = np.arange(seq_len, dtype=np.float32)[:, None] * inv_freq[None, :]
    cos, sin = np.cos(angle), np.sin(angle)
    return np.concatenate([cos, cos], axis=1), np.concatenate([-sin, sin], axis=1)


def relay_kernel(heads, acc, *refs):
    n_ref, sources, o_ref = refs[0], refs[1:-1], refs[-1]
    depth, head_dim = o_ref.shape[0], sources[0].shape[1]
    block = 256
    span = block // heads
    row = lax.broadcasted_iota(jnp.int32, (block, block), 0)
    col = lax.broadcasted_iota(jnp.int32, (block, block), 1)
    order = jnp.where(col == (row % span) * heads + row // span, 1.0, 0.0).astype(BF16)
    for g in range(depth // span):
        for w, ref in enumerate(sources):
            moved = jnp.dot(order, ref[g * block:(g + 1) * block, :], preferred_element_type=F32).astype(BF16)
            for k in range(heads):
                lane = (w * heads + k) * head_dim
                o_ref[g * span:(g + 1) * span, lane:lane + head_dim] = moved[k * span:(k + 1) * span]
    wide = 512
    for t in range(o_ref.shape[1] // wide):
        cols = pl.ds(t * wide, wide)
        acc[:, cols] += jnp.dot(n_ref[...], o_ref[:, cols], preferred_element_type=F32)


TILE = 256
CHUNKS = 4
PAIRS = 2
E_BLOCKS = 2
NT_SLOTS = 3
NN_SLOTS = 4


def layer_kernel(tp, ep, heads, wq, wk, wv, w_out, x, gain, wg, wu, wd, eg, eu, ed, wr, ids, slots, cos_ref, sin_ref,
                 out, n, send, wqkv, c_l, c_r, c_o, a_l, a_r, a_o, wx, recv, y, back,
                 route, r1, r2, a_own, a_mine, out_q, wb1, wb2, wb3,
                 send_sem, recv_sem, dsend, drecv, ysend, yrecv, ysem, wsend, wrecv, sem1, sem2, sem3, lsem, osem):
    seq, d_model = out.shape
    rows = seq // CHUNKS
    quarter = rows // tp
    width = d_model // tp
    slots_all = recv.shape[0]
    top_k = ids.shape[0]
    sub = slots_all // ep
    me = lax.axis_index('tp')
    my_e = lax.axis_index('ep')
    right, left, far = lax.rem(me + 1, tp), lax.rem(me + tp - 1, tp), lax.rem(me + 2, tp)

    barrier = pltpu.get_barrier_semaphore()
    for peer in (right, far, left):
        pl.semaphore_signal(barrier, inc=1, device_id={'tp': peer}, device_id_type=MESH)
    for k in range(1, ep):
        pl.semaphore_signal(barrier, inc=1, device_id={'ep': lax.rem(my_e + k, ep)}, device_id_type=MESH)
    pl.semaphore_wait(barrier, 3 + ep - 1)

    def at(start, size, align):
        return pl.ds(pl.multiple_of(start, align), size)

    held = {}

    def remote(kind, c, d, src, dst):
        return pltpu.make_async_remote_copy(
            src_ref=src, dst_ref=dst, send_sem=send_sem.at[kind, c, d], recv_sem=recv_sem.at[kind, c, d],
            device_id={'tp': (right, left)[d]}, device_id_type=MESH)

    half = rows // 2

    def c_first(c, d):
        piece = at(c * rows, rows, rows)
        return remote(0, c, d, held['qkv'].at[piece, pl.ds(0, width)], (c_l, c_r)[d].at[piece, :])

    def c_second(c, d):
        piece = at(c * rows + d * half, half, half)
        return remote(1, c, d, (c_l, c_r)[d].at[piece, :], c_o.at[piece, :])

    def a_first(c, d):
        piece = at(c * rows, rows, rows)
        return remote(2, c, d, a_own.at[piece, :], (a_l, a_r)[d].at[piece, :])

    def a_second(c, d):
        piece = at(c * rows + d * half, half, half)
        return remote(3, c, d, (a_l, a_r)[d].at[piece, :], a_o.at[piece, :])

    q_half = quarter // 2

    def r_first(c, d):
        return remote(4, c, d, held['fbuf'].at[lax.rem(c, 2), at(far * quarter + d * q_half, q_half, q_half), :], r1.at[lax.rem(c, 2), d])

    def r_second(c, d):
        return remote(5, c, d, held['fbuf'].at[lax.rem(c, 2), at((right, left)[d] * quarter, quarter, quarter), :], r2.at[lax.rem(c, 2), d])

    def o_half(kind, c, d, part):
        rows_of = c * rows + me * quarter + part * q_half
        return remote(kind, c, d, out_q.at[c, pl.ds(part * q_half, q_half), :], out.at[at(rows_of, q_half, q_half), :])

    def o_first(c, d):
        return o_half(6, c, d, d)

    def o_other(c, d):
        return o_half(8, c, d, 1 - d)

    def o_second(c, d):
        piece = at(c * rows + (left, right)[d] * quarter + d * q_half, q_half, q_half)
        return remote(7, c, d, out.at[piece, :], out.at[piece, :])

    def start(make, c):
        make(c, 0).start()
        make(c, 1).start()

    def arrived(make, c):
        make(c, 0).wait_recv()
        make(c, 1).wait_recv()

    def sent(make, c):
        make(c, 0).wait_send()
        make(c, 1).wait_send()

    share = w_out.shape[0] // 2
    core = lax.rem(my_e, 2)
    core_rows = at(core * share, share, share)

    def w_first(k):
        peer = lax.rem(me + k, tp)
        return pltpu.make_async_remote_copy(
            src_ref=w_out.at[core_rows, at(peer * width, width, width)], dst_ref=wx.at[me, core_rows, :],
            send_sem=wsend.at[0, k], recv_sem=wrecv.at[0, k], device_id={'tp': peer}, device_id_type=MESH)

    def w_second(k):
        piece = wx.at[lax.rem(me + tp - k, tp), core_rows, :]
        return pltpu.make_async_remote_copy(
            src_ref=piece, dst_ref=piece, send_sem=wsend.at[1, k], recv_sem=wrecv.at[1, k],
            device_id={'ep': my_e + 1 - 2 * core}, device_id_type=MESH)

    def w_start():
        for k in range(1, tp):
            w_first(k).start()

    def w_pair():
        for k in range(1, tp):
            w_first(k).wait_recv()
            w_second(k).start()

    def w_done():
        for k in range(1, tp):
            w_second(k).wait_recv()

    def w_sent():
        for k in range(1, tp):
            w_first(k).wait_send()
            w_second(k).wait_send()

    class Pair:
        def __init__(self, wa, wb):
            self.refs = (wa, wb)
            self.full, self.tail = wa.shape[0] // TILE, wa.shape[0] % TILE
            self.tiles = self.full + (self.tail > 0)

        def copies(self, i, slot, n=TILE):
            return [pltpu.make_async_copy(w.at[at(i * TILE, n, 32), :], wb1.at[slot, k, pl.ds(0, n), :], sem1.at[slot, k]) for k, w in enumerate(self.refs)]

        def go(self, i, slot, n=TILE):
            for cp in self.copies(i, slot, n):
                cp.start()

        def ready(self, i, slot, n=TILE):
            for cp in self.copies(i, slot, n):
                cp.wait()

    nt_ahead = NT_SLOTS - 1

    def gate_up(lhs, h, pair, base, then, mid=None):
        full, tail = pair.full, pair.tail

        def product(slot, n):
            dims = (((1,), (1,)), ((), ()))
            gate = lax.dot_general(lhs[:h.shape[0], :], wb1[slot, 0, :n, :], dims, preferred_element_type=F32)
            up = lax.dot_general(lhs[:h.shape[0], :], wb1[slot, 1, :n, :], dims, preferred_element_type=F32)
            return (jax.nn.silu(gate) * up).astype(BF16)

        def step(i, carry):
            nxt = i + nt_ahead
            ahead = lax.rem(base + nxt, NT_SLOTS)
            pl.when(nxt < full)(lambda: pair.go(nxt, ahead))
            if tail:
                pl.when(nxt == full)(lambda: pair.go(full, ahead, tail))
            pl.when(nxt >= pair.tiles)(lambda: then(nxt - pair.tiles, ahead))
            slot = lax.rem(base + i, NT_SLOTS)
            pair.ready(i, slot)
            h[:, at(i * TILE, TILE, TILE)] = product(slot, TILE)
            if mid is not None:
                pl.when(i == full // 2)(mid)
            return carry

        lax.fori_loop(0, full, step, 0)
        if tail:
            then(full + nt_ahead - pair.tiles, lax.rem(base + full + nt_ahead, NT_SLOTS))
            slot = lax.rem(base + full, NT_SLOTS)
            pair.ready(full, slot, tail)
            h[:, full * TILE:full * TILE + tail] = product(slot, tail)

    nn_ahead = NN_SLOTS - 1

    def go(fetch, i, slot):
        for cp in fetch(i, slot):
            cp.start()

    def prime(fetch):
        for j in range(nn_ahead):
            go(fetch, j, j)

    def columns(left_ref, m, depth, tiles, fetch, use, then=None, off=0):
        def step(i, carry):
            nxt = i + nn_ahead
            ahead = lax.rem(nxt, NN_SLOTS)
            pl.when(nxt < tiles)(lambda: go(fetch, nxt, ahead))
            if then is not None:
                pl.when(nxt >= tiles)(lambda: then(nxt - tiles, ahead))
            slot = lax.rem(i, NN_SLOTS)
            for cp in fetch(i, slot):
                cp.wait()
            use(i, slot, jnp.dot(left_ref[off:off + m, :depth], wb2[slot, :depth, :], preferred_element_type=F32))
            return carry

        lax.fori_loop(0, tiles, step, 0)

    def whole_depth(w):
        def fetch(i, slot):
            return [pltpu.make_async_copy(w.at[:, at(i * TILE, TILE, TILE)], wb2.at[slot, pl.ds(0, w.shape[0]), :], sem2.at[slot, 0])]
        return fetch

    experts_in = Pair(eg, eu)
    ffn_in = Pair(wg, wu)
    from_qkv, from_ed, from_wd = whole_depth(wqkv), whole_depth(ed), whole_depth(wd)

    def from_out(i, slot):
        cols = at(i * TILE, TILE, TILE)
        own = pltpu.make_async_copy(w_out.at[:, at(me * width + i * TILE, TILE, TILE)], wb2.at[slot, at(me * width, width, width), :], sem2.at[slot, 0])
        rest = [pltpu.make_async_copy(wx.at[who, :, cols], wb2.at[slot, at(who * width, width, width), :], sem2.at[slot, k])
                for k, who in ((1, right), (2, far), (3, left))]
        return [own] + rest

    pair_rows = seq // PAIRS
    e_rows = slots_all // E_BLOCKS

    def c_forward(c):
        arrived(c_first, c)
        start(c_second, c)

    chips = ep // 2
    my_chip = my_e // 2
    order = sorted(((m, flip) for m in range(chips) for flip in range(2)), key=lambda v: (-min(v[0], chips - v[0]), -v[1]))
    place = {v: q for q, v in enumerate(order)}
    others = range(ep - 1)

    def peer_of(q):
        m, flip = order[q]
        return 2 * lax.rem(my_chip + m, chips) + (1 - core if flip else core)

    def back_place(q):
        m, flip = order[q]
        return place[((chips - m) % chips, flip)]

    def d_copy(q):
        peer = peer_of(q)
        return pltpu.make_async_remote_copy(
            src_ref=send.at[at(peer * sub, sub, sub), :], dst_ref=recv.at[pl.ds(back_place(q) * sub, sub), :],
            send_sem=dsend.at[q], recv_sem=drecv.at[q], device_id={'ep': peer}, device_id_type=MESH)

    own_rows = at(my_e * sub, sub, sub)

    def y_copy(q):
        return pltpu.make_async_remote_copy(
            src_ref=y.at[pl.ds(q * sub, sub), :], dst_ref=back.at[own_rows, :],
            send_sem=ysend.at[q], recv_sem=yrecv.at[q], device_id={'ep': peer_of(q)}, device_id_type=MESH)


    def y_back():
        for q in others:
            y_copy(q).wait_recv()

    def a_forward(c):
        arrived(a_first, c)
        start(a_second, c)

    w_start()

    def prepare(u, pick, x_in, n_out, piled):
        size = x_in.shape[1]
        blocks = seq // size

        def x_get(i, k):
            return pltpu.make_async_copy(x.at[at(i * size, size, size), :], x_in.at[k], sem2.at[k, 0])

        def n_put(i, k):
            return pltpu.make_async_copy(n_out.at[k], n.at[at(i * size, size, size), :], sem3.at[k])

        x_get(0, 0).start()

        def norm(i, carry):
            k = lax.rem(i, 2)
            pl.when(i + 1 < blocks)(lambda: x_get(i + 1, 1 - k).start())
            pl.when(i >= 2)(lambda: n_put(i - 2, k).wait())
            x_get(i, k).wait()
            mine = at(i * size, size, size)
            val = x_in[k].astype(F32)
            unit = val * lax.rsqrt(jnp.mean(val * val, axis=-1, keepdims=True) + EPS)
            n_out[k] = (unit * gain[0:1, :]).astype(BF16)
            n_put(i, k).start()
            row = (unit * gain[1:2, :]).astype(BF16)
            u[mine, :] = row
            logits = lax.dot_general(wr[...], row, (((1,), (1,)), ((), ())), preferred_element_type=F32)
            expert = lax.broadcasted_iota(jnp.int32, logits.shape, 0)
            picked = [jnp.sum(jnp.where(expert == ids[j:j + 1, mine], logits, 0.0), axis=0, keepdims=True) for j in range(top_k)]
            top = functools.reduce(jnp.maximum, picked)
            weights = [jnp.exp(p - top) for p in picked]
            total = sum(weights)
            for j in range(top_k):
                route[top_k + j:top_k + j + 1, mine] = weights[j] / total
            return carry
        lax.fori_loop(0, blocks, norm, 0)
        rows_all = lax.broadcasted_iota(jnp.int32, pick.shape, 0)
        hit = None
        for j in range(top_k):
            slot = slots[j:j + 1, :]
            row_of = jnp.where(lax.rem(slot, tp) == me, ids[j:j + 1, :] * sub + lax.div(slot, tp), -1)
            route[j:j + 1, :] = row_of.astype(F32)
            match = rows_all == row_of
            hit = match if hit is None else hit | match
        pick[...] = jnp.where(hit, 1.0, 0.0).astype(BF16)
        cols = piled.shape[2]
        parts = d_model // cols

        def put(i, k):
            return pltpu.make_async_copy(piled.at[k], send.at[:, at(i * cols, cols, cols)], sem1.at[k, 0])

        def gather(i, carry):
            k = lax.rem(i, 2)
            pl.when(i >= 2)(lambda: put(i - 2, k).wait())
            piled[k] = jnp.dot(pick[...], u[:, at(i * cols, cols, cols)], preferred_element_type=F32).astype(BF16)
            put(i, k).start()
            return carry
        lax.fori_loop(0, parts, gather, 0)
        for i in range(parts - 2, parts):
            put(i, i % 2).wait()
        for i in range(blocks - 2, blocks):
            n_put(i, i % 2).wait()

    tokens = 128
    pl.run_scoped(
        prepare, pltpu.VMEM((seq, d_model), BF16), pltpu.VMEM((slots_all, seq), BF16), pltpu.VMEM((2, tokens, d_model), BF16),
        pltpu.VMEM((2, tokens, d_model), BF16), pltpu.VMEM((2, slots_all, 512), BF16))
    for q in others:
        d_copy(q).start()

    head_dim = width // heads
    low = head_dim // 2

    def first_half(lhs, he, qkv, ystage, acc):
        held['qkv'] = qkv

        def n_load(p):
            return pltpu.make_async_copy(n.at[pl.ds(p * pair_rows, pair_rows), :], lhs.at[pl.ds(0, pair_rows), :], lsem.at[0])

        def rotate(val, piece):
            parts = []
            for k in range(TILE // head_dim):
                one = val[:, k * head_dim:(k + 1) * head_dim]
                parts.append(one * cos_ref[piece, :] + pltpu.roll(one, low, 1) * sin_ref[piece, :])
            return jnp.concatenate(parts, axis=1)

        def settle(piece, i, val):
            val = jnp.where(i < 2 * width // TILE, rotate(val, piece), val)
            qkv[piece, at(i * TILE, TILE, TILE)] = val.astype(BF16)

        def project_in(start_row, count, off, follow, between=None):
            piece = pl.ds(start_row, count)

            def keep(i, slot, val):
                settle(piece, i, val)

            def then(i, slot):
                if between is not None:
                    pl.when(i == 0)(between)
                go(follow, i, slot)
            columns(lhs, count, d_model, 3 * width // TILE, from_qkv, keep, then, off)

        def attend(c):
            base = c * rows
            keys = base + rows
            dims = (((1,), (1,)), ((), ()))

            def two(g, carry):
                for k in range(2):
                    hh = 2 * g + k
                    lane = lambda off: at(off + hh * head_dim, head_dim, head_dim)
                    query = qkv[base:keys, lane(0)]
                    scores = lax.dot_general(query, qkv[base:keys, lane(width)], dims, preferred_element_type=F32)
                    row = lax.broadcasted_iota(jnp.int32, scores.shape, 0)
                    col = lax.broadcasted_iota(jnp.int32, scores.shape, 1)
                    scores = jnp.where(row >= col, scores, -1e30)
                    if c:
                        before = lax.dot_general(query, qkv[0:base, lane(width)], dims, preferred_element_type=F32)
                        scores = jnp.concatenate([before, scores], axis=1)
                    top = jnp.max(scores, axis=1, keepdims=True)
                    prob = jnp.exp2((scores - top) * (head_dim ** -0.5 * LOG2E))
                    prob = (prob * (1.0 / jnp.sum(prob, axis=1, keepdims=True))).astype(BF16)
                    qkv[base:keys, lane(0)] = jnp.dot(prob, qkv[0:keys, lane(2 * width)], preferred_element_type=F32).astype(BF16)
                return carry
            lax.fori_loop(0, heads // 2, two, 0)

        def x_load(b):
            far = e_rows - (sub if b == E_BLOCKS - 1 else 0)
            copies = [pltpu.make_async_copy(recv.at[pl.ds(b * e_rows, far), :], lhs.at[pl.ds(0, far), :], lsem.at[0])]
            if far < e_rows:
                copies.append(pltpu.make_async_copy(send.at[own_rows, :], lhs.at[pl.ds(far, sub), :], lsem.at[1]))
            return copies

        def expert(b, mid):
            loads = x_load(b)
            for cp in loads:
                cp.start()
            for cp in loads:
                cp.wait()
            last = b == E_BLOCKS - 1
            gate_up(lhs, he, experts_in, b * experts_in.tiles, ffn_in.go if last else experts_in.go, mid)
            tiles = d_model // TILE

            far = e_rows - (sub if last else 0)

            def puts(i):
                k = lax.rem(i, 2)
                cols = at(i * TILE, TILE, TILE)
                copies = [pltpu.make_async_copy(ystage.at[k, pl.ds(0, far), :], y.at[pl.ds(b * e_rows, far), cols], ysem.at[k, 0])]
                if last:
                    copies.append(pltpu.make_async_copy(ystage.at[k, pl.ds(far, sub), :], back.at[own_rows, cols], ysem.at[k, 1]))
                return copies

            def put(i):
                for cp in puts(i):
                    cp.start()

            def put_wait(i):
                for cp in puts(i):
                    cp.wait()

            def keep(i, slot, acc):
                pl.when(i >= 2)(lambda: put_wait(i - 2))
                ystage[lax.rem(i, 2)] = acc.astype(BF16)
                put(i)
            follow = from_out if last else from_ed
            columns(he, e_rows, ed.shape[0], tiles, from_ed, keep, lambda i, slot: go(follow, i, slot))
            put_wait(tiles - 2)
            put_wait(tiles - 1)
            span = ep // E_BLOCKS
            for k in range(b * span, (b + 1) * span):
                if k < ep - 1:
                    y_copy(k).start()

        def project_out(p):
            for k in range(CHUNKS // PAIRS):
                arrived(c_second, p * (CHUNKS // PAIRS) + k)
            piece = pl.ds(p * pair_rows, pair_rows)
            here = pl.ds(0, pair_rows)
            loads = [pltpu.make_async_copy(src.at[piece, :], lhs.at[here, at(who * width, width, width)], lsem.at[k])
                     for k, (src, who) in enumerate(((c_r, right), (c_o, far), (c_l, left)))]
            loads.append(pltpu.make_async_copy(x.at[piece, at(me * width, width, width)], a_own.at[piece, :], lsem.at[4]))
            for cp in loads:
                cp.start()
            lhs[here, at(me * width, width, width)] = qkv[piece, 0:width]
            for cp in loads:
                cp.wait()

            def keep(i, slot, acc):
                block = (piece, at(i * TILE, TILE, TILE))
                a_own[block] = (a_own[block].astype(F32) + acc).astype(BF16)
            follow = from_ed if p < PAIRS - 1 else from_wd
            columns(lhs, pair_rows, d_model, width // TILE, from_out, keep, lambda i, slot: go(follow, i, slot))

        second_load = pltpu.make_async_copy(n.at[pl.ds(rows, rows), :], lhs.at[pl.ds(rows, rows), :], lsem.at[0])
        second_load.start()
        acc[...] = jnp.zeros_like(acc)
        depth_block = 256
        pltpu.emit_pipeline(
            functools.partial(relay_kernel, heads, acc),
            grid=(d_model // depth_block,),
            in_specs=[pl.BlockSpec((rows, depth_block), lambda i: (0, i), pipeline_mode=pl.Buffered(3))]
            + [pl.BlockSpec((depth_block * heads, head_dim), lambda i: (i, 0), pipeline_mode=pl.Buffered(3))] * 3,
            out_specs=[pl.BlockSpec((depth_block, 3 * width), lambda i: (i, 0))],
        )(n, wq, wk, wv, wqkv)
        prime(from_qkv)

        def settle_first(i, carry):
            settle(pl.ds(0, rows), i, acc[:, at(i * TILE, TILE, TILE)])
            return carry
        lax.fori_loop(0, 3 * width // TILE, settle_first, 0)
        attend(0)
        start(c_first, 0)
        second_load.wait()
        project_in(rows, rows, rows, from_qkv)
        n_load(1).start()
        attend(1)
        start(c_first, 1)
        for k in range(nt_ahead):
            experts_in.go(k, k)
        w_pair()
        n_load(1).wait()
        c_forward(0)
        project_in(2 * rows, 2 * rows, 0, from_out, w_done)
        c_forward(1)
        attend(2)
        start(c_first, 2)
        attend(3)
        start(c_first, 3)
        project_out(0)
        start(a_first, 0)
        for q in others:
            d_copy(q).wait_recv()
        expert(0, lambda: c_forward(2))
        c_forward(3)

        def late():
            a_forward(0)
            start(a_first, 1)
        expert(1, late)
        project_out(1)
        for c in range(CHUNKS):
            sent(c_first, c)

    pl.run_scoped(
        first_half, pltpu.VMEM((max(pair_rows, e_rows), d_model), BF16), pltpu.VMEM((e_rows, ed.shape[0]), BF16),
        pltpu.VMEM((seq, 3 * width), BF16), pltpu.VMEM((2, e_rows, TILE), BF16),
        pltpu.VMEM((rows, 3 * width), F32))
    start(a_first, 2)

    def second_half(lhs, h, fbuf, a_in, sel, gates):
        held['fbuf'] = fbuf

        def reduce_on(c):
            for d, who in ((0, right), (1, left)):
                r_first(c, d).wait_recv()

                def add(k, carry, d=d, who=who):
                    block = (lax.rem(c, 2), at(who * quarter + d * q_half + k * 8, 8, 8), slice(None))
                    fbuf[block] = fbuf[block] + r1[lax.rem(c, 2), d, at(k * 8, 8, 8), :]
                    return carry
                lax.fori_loop(0, q_half // 8, add, 0)
            start(r_second, c)

        def o_local(c):
            return pltpu.make_async_copy(out_q.at[c], out.at[at(c * rows + me * quarter, quarter, quarter), :], osem.at[c])

        def finish(c):
            arrived(r_second, c)

            def add(k, carry):
                part = at(k * 16, 16, 16)
                total = fbuf[lax.rem(c, 2), at(me * quarter + k * 16, 16, 16), :] + (r2[lax.rem(c, 2), 0, part, :] + r2[lax.rem(c, 2), 1, part, :])
                out_q[c, part, :] = (a_mine[c, part, :].astype(F32) + total).astype(BF16)
                return carry
            lax.fori_loop(0, quarter // 16, add, 0)
            start(o_first, c)
            start(o_other, c)
            o_local(c).start()

        def o_forward(c):
            arrived(o_first, c)
            start(o_second, c)

        def from_back(i, slot):
            return pltpu.make_async_copy(back.at[:, at(i * TILE, TILE, TILE)], wb3.at[slot], sem3.at[slot])

        def copies_prime():
            for k in range(nn_ahead):
                from_back(k, k).start()

        def combine(c):
            tiles = d_model // TILE

            def step(i, carry):
                nxt = i + nn_ahead
                pl.when(nxt < tiles)(lambda: from_back(nxt, lax.rem(nxt, NN_SLOTS)).start())
                slot = lax.rem(i, NN_SLOTS)
                from_back(i, slot).wait()
                copies = jnp.dot(sel[...], wb3[slot], preferred_element_type=F32)
                block = (lax.rem(c, 2), slice(None), at(i * TILE, TILE, TILE))
                total = fbuf[block]
                for j in range(top_k):
                    total = total + gates[:, j:j + 1] * copies[j * rows:(j + 1) * rows]
                fbuf[block] = total
                return carry
            lax.fori_loop(0, tiles, step, 0)

        def ffn(c, carry):
            arrived(a_second, c)
            piece = at(c * rows, rows, rows)
            loads = [pltpu.make_async_copy(src.at[piece, :], a_in.at[k], lsem.at[k]) for k, src in enumerate((a_r, a_o, a_l))]
            for cp in loads:
                cp.start()
            for cp in loads:
                cp.wait()
            parts = ((None, me), (0, right), (1, far), (2, left))

            def norm(k, carry):
                block = at(k * 16, 16, 16)
                vals = [(a_own[at(c * rows + k * 16, 16, 16), :] if p is None else a_in[p, block, :]).astype(F32) for p, _ in parts]
                square = sum(jnp.sum(v * v, axis=1, keepdims=True) for v in vals)
                inv = lax.rsqrt(square / d_model + EPS)
                for v, (_, who) in zip(vals, parts):
                    cols = at(who * width, width, width)
                    lhs[block, cols] = (v * inv * gain[2:3, cols]).astype(BF16)
                return carry
            lax.fori_loop(0, rows // 16, norm, 0)
            for p, who in parts:
                mine = at(me * quarter, quarter, quarter)
                val = a_own[at(c * rows + me * quarter, quarter, quarter), :] if p is None else a_in[p, mine, :]
                a_mine[c, :, at(who * width, width, width)] = val
            table = jnp.transpose(route[:, piece])
            lane = lax.broadcasted_iota(jnp.int32, (rows, slots_all), 1).astype(F32)
            for j in range(top_k):
                sel[j * rows:(j + 1) * rows, :] = jnp.where(lane == table[:, j:j + 1], 1.0, 0.0).astype(BF16)
                gates[:, j:j + 1] = table[:, top_k + j:top_k + j + 1]

            def mid():
                @pl.when(c == 0)
                def _():
                    a_forward(1)
                    start(a_first, 3)
                pl.when(c >= 1)(lambda: reduce_on(c - 1))
            def after(i, slot):
                pl.when(c < CHUNKS - 1)(lambda: ffn_in.go(i, slot))
            gate_up(lhs, h, ffn_in, E_BLOCKS * experts_in.tiles + c * ffn_in.tiles, after, mid)
            pl.when(c == 0)(lambda: a_forward(2))

            @pl.when(c >= 2)
            def _():
                o_forward(c - 2)
                sent(r_first, c - 2)
                sent(r_second, c - 2)

            def keep(i, slot, acc):
                fbuf[lax.rem(c, 2), :, at(i * TILE, TILE, TILE)] = acc

            def then(i, slot):
                pl.when(c < CHUNKS - 1)(lambda: go(from_wd, i, slot))
            pl.when(c > 0)(copies_prime)
            columns(h, rows, wd.shape[0], d_model // TILE, from_wd, keep, then)

            @pl.when(c == 0)
            def _():
                a_forward(3)
                y_back()
                copies_prime()
            combine(c)
            start(r_first, c)
            pl.when(c >= 1)(lambda: finish(c - 1))
            return carry
        lax.fori_loop(0, CHUNKS, ffn, 0)
        reduce_on(CHUNKS - 1)
        o_forward(CHUNKS - 2)
        finish(CHUNKS - 1)
        o_forward(CHUNKS - 1)

        def drain(c, carry):
            arrived(o_second, c)
            arrived(o_other, c)
            o_local(c).wait()
            for make in (c_second, a_first, a_second, o_first, o_other, o_second):
                sent(make, c)

            @pl.when(c >= CHUNKS - 2)
            def _():
                sent(r_first, c)
                sent(r_second, c)
            return carry
        lax.fori_loop(0, CHUNKS, drain, 0)
        for q in others:
            d_copy(q).wait_send()
            y_copy(q).wait_send()
        w_sent()

    pl.run_scoped(
        second_half, pltpu.VMEM((rows, d_model), BF16), pltpu.VMEM((rows, wd.shape[0]), BF16), pltpu.VMEM((2, rows, d_model), F32),
        pltpu.VMEM((3, rows, width), BF16), pltpu.VMEM((top_k * rows, slots_all), BF16), pltpu.VMEM((rows, top_k), F32))


def fused_layer(tp, ep, heads, slots_all, wq, wk, wv, w_out, x, gains, wg, wu, wd, eg, eu, ed, router, ids, slots, cos, sin):
    seq, d_model = x.shape
    rows = seq // CHUNKS
    quarter = rows // tp
    width = d_model // tp
    hidden = wd.shape[0]
    any_spec = pl.BlockSpec(memory_space=pl.ANY)
    vmem_spec = pl.BlockSpec(memory_space=pltpu.VMEM)
    part = jax.ShapeDtypeStruct((seq, width), BF16)
    copies = jax.ShapeDtypeStruct((slots_all, d_model), BF16)
    outs = pl.pallas_call(
        functools.partial(layer_kernel, tp, ep, heads),
        out_shape=[jax.ShapeDtypeStruct((seq, d_model), BF16)] * 2 + [copies, jax.ShapeDtypeStruct((d_model, 3 * width), BF16)] + [part] * 6
        + [jax.ShapeDtypeStruct((tp, w_out.shape[0], width), BF16)] + [copies] * 3,
        in_specs=[any_spec] * 5 + [vmem_spec] + [any_spec] * 6 + [vmem_spec] * 5,
        out_specs=[any_spec] * 14,
        scratch_shapes=[
            pltpu.VMEM((8, seq), F32),
            pltpu.VMEM((2, 2, quarter // 2, d_model), F32),
            pltpu.VMEM((2, 2, quarter, d_model), F32),
            pltpu.VMEM((seq, width), BF16),
            pltpu.VMEM((CHUNKS, quarter, d_model), BF16),
            pltpu.VMEM((CHUNKS, quarter, d_model), BF16),
            pltpu.VMEM((NT_SLOTS, 2, TILE, d_model), BF16),
            pltpu.VMEM((NN_SLOTS, d_model, TILE), BF16),
            pltpu.VMEM((NN_SLOTS, slots_all, TILE), BF16),
            pltpu.SemaphoreType.DMA((9, CHUNKS, 2)),
            pltpu.SemaphoreType.DMA((9, CHUNKS, 2)),
            pltpu.SemaphoreType.DMA((ep,)),
            pltpu.SemaphoreType.DMA((ep,)),
            pltpu.SemaphoreType.DMA((ep,)),
            pltpu.SemaphoreType.DMA((ep,)),
            pltpu.SemaphoreType.DMA((2, 2)),
            pltpu.SemaphoreType.DMA((2, tp)),
            pltpu.SemaphoreType.DMA((2, tp)),
            pltpu.SemaphoreType.DMA((NT_SLOTS, 2)),
            pltpu.SemaphoreType.DMA((NN_SLOTS, 4)),
            pltpu.SemaphoreType.DMA((NN_SLOTS,)),
            pltpu.SemaphoreType.DMA((5,)),
            pltpu.SemaphoreType.DMA((CHUNKS,)),
        ],
        compiler_params=pltpu.CompilerParams(collective_id=0, has_side_effects=True, vmem_limit_bytes=67043328),
        cost_estimate=pl.CostEstimate(flops=6 * seq * d_model * hidden, bytes_accessed=300 * 2 ** 20, transcendentals=seq * hidden),
    )(wq, wk, wv, w_out, x, gains, wg, wu, wd, eg, eu, ed, router, ids, slots, cos, sin)
    return outs[0]


def solution(mesh):
    tok_spec = P(('dp', 'ep'), None, None)
    col_spec = P(None, 'tp', None)
    exp_spec = P('ep', None, None)
    in_specs = (tok_spec, tok_spec, tok_spec, P(None), col_spec, col_spec, col_spec, P('tp', None, None), P(None), P(None, 'tp'), P(None, 'tp'), P('tp', None), P(None), P(None, None), exp_spec, exp_spec, exp_spec)
    tp = mesh.shape['tp']
    ep = mesh.shape['ep']

    def layer_local(hidden_in, expert_ids, slot_ids, attn_gain, w_query, w_key, w_value, w_out, ffn_gain, w_gate, w_up, w_down, moe_gain, w_router, exp_gate, exp_up, exp_down):
        _, seq, d_model = hidden_in.shape
        heads, head_dim = w_query.shape[1:]
        experts = w_router.shape[1]
        top_k = expert_ids.shape[2]
        cap = 3 * seq * top_k // (2 * experts)
        sub = cap // tp
        x = hidden_in[0]
        gains = jnp.stack([attn_gain, moe_gain, ffn_gain]).astype(F32)
        cos, sin = rope_tables(seq, head_dim)
        flat = lambda w: w.reshape(d_model * heads, head_dim)
        out = fused_layer(tp, ep, heads, experts * sub, flat(w_query), flat(w_key), flat(w_value), w_out.reshape(heads * head_dim, d_model), x,
                          gains, w_gate.T, w_up.T, w_down, exp_gate[0].T, exp_up[0].T, exp_down[0],
                          w_router.T, expert_ids[0].T, slot_ids[0].T, cos, sin)
        return out[None]

    return jax.shard_map(layer_local, mesh=mesh, in_specs=in_specs, out_specs=tok_spec, check_vma=False)
```

```python
import functools

import jax
import jax.numpy as jnp
import numpy as np
from jax import lax
from jax.experimental import pallas as pl
from jax.experimental.pallas import tpu as pltpu
from jax.sharding import PartitionSpec as P

EPS = 1e-6
ROPE_BASE = 10000.0
LOG2E = 1.4426950408889634
MESH = pl.DeviceIdType.MESH
F32, BF16 = jnp.float32, jnp.bfloat16


def rope_tables(seq_len, head_dim):
    inv_freq = np.float32(ROPE_BASE) ** (-np.arange(head_dim // 2, dtype=np.float32) * np.float32(2.0 / head_dim))
    angle = np.arange(seq_len, dtype=np.float32)[:, None] * inv_freq[None, :]
    cos, sin = np.cos(angle), np.sin(angle)
    return np.concatenate([cos, cos], axis=1), np.concatenate([-sin, sin], axis=1)


def relay_kernel(heads, acc, *refs):
    n_ref, sources, o_ref = refs[0], refs[1:-1], refs[-1]
    depth, head_dim = o_ref.shape[0], sources[0].shape[1]
    block = 256
    span = block // heads
    row = lax.broadcasted_iota(jnp.int32, (block, block), 0)
    col = lax.broadcasted_iota(jnp.int32, (block, block), 1)
    order = jnp.where(col == (row % span) * heads + row // span, 1.0, 0.0).astype(BF16)
    pieces = [(g, w) for g in range(depth // span) for w in range(len(sources))]
    for first, second in zip(pieces[::2], pieces[1::2]):
        both = jnp.concatenate([sources[w][g * block:(g + 1) * block, :] for g, w in (first, second)], axis=1)
        moved = jnp.dot(order, both, preferred_element_type=F32).astype(BF16)
        for part, (g, w) in enumerate((first, second)):
            for k in range(heads):
                lane = (w * heads + k) * head_dim
                o_ref[g * span:(g + 1) * span, lane:lane + head_dim] = moved[k * span:(k + 1) * span, part * head_dim:(part + 1) * head_dim]
    wide = 512
    for t in range(o_ref.shape[1] // wide):
        cols = pl.ds(t * wide, wide)
        acc[:, cols] += jnp.dot(n_ref[...], o_ref[:, cols], preferred_element_type=F32)


TILE = 256
CHUNKS = 4
PAIRS = 2
E_BLOCKS = 2
NT_SLOTS = 3
NN_SLOTS = 4


def layer_kernel(tp, ep, heads, wq, wk, wv, w_out, x, gain_flat, wg, wu, wd, eg, eu, ed, wr, ids, slots, cos_ref, sin_ref,
                 out, n, send, wqkv, c_l, c_r, c_o, a_l, a_r, a_o, wx, recv, y, back,
                 gain, route, r1, r2, a_own, a_mine, out_q, wb1, wb2, wb3,
                 send_sem, recv_sem, dsend, drecv, ysend, yrecv, ysem, wsend, wrecv, sem1, sem2, sem3, lsem, osem):
    seq, d_model = out.shape
    rows = seq // CHUNKS
    quarter = rows // tp
    width = d_model // tp
    slots_all = recv.shape[0]
    top_k = ids.shape[0]
    sub = slots_all // ep
    me = lax.axis_index('tp')
    my_e = lax.axis_index('ep')
    right, left, far = lax.rem(me + 1, tp), lax.rem(me + tp - 1, tp), lax.rem(me + 2, tp)

    barrier = pltpu.get_barrier_semaphore()
    for peer in (right, far, left):
        pl.semaphore_signal(barrier, inc=1, device_id={'tp': peer}, device_id_type=MESH)
    for k in range(1, ep):
        pl.semaphore_signal(barrier, inc=1, device_id={'ep': lax.rem(my_e + k, ep)}, device_id_type=MESH)
    pl.semaphore_wait(barrier, 3 + ep - 1)

    def at(start, size, align):
        return pl.ds(pl.multiple_of(start, align), size)

    held = {}

    def remote(kind, c, d, src, dst):
        return pltpu.make_async_remote_copy(
            src_ref=src, dst_ref=dst, send_sem=send_sem.at[kind, c, d], recv_sem=recv_sem.at[kind, c, d],
            device_id={'tp': (right, left)[d]}, device_id_type=MESH)

    half = rows // 2

    def c_first(c, d):
        piece = at(c * rows, rows, rows)
        return remote(0, c, d, held['qkv'].at[piece, pl.ds(0, width)], (c_l, c_r)[d].at[piece, :])

    def c_second(c, d):
        piece = at(c * rows + d * half, half, half)
        return remote(1, c, d, (c_l, c_r)[d].at[piece, :], c_o.at[piece, :])

    def a_first(c, d):
        piece = at(c * rows, rows, rows)
        return remote(2, c, d, a_own.at[piece, :], (a_l, a_r)[d].at[piece, :])

    def a_second(c, d):
        piece = at(c * rows + d * half, half, half)
        return remote(3, c, d, (a_l, a_r)[d].at[piece, :], a_o.at[piece, :])

    q_half = quarter // 2

    def r_first(c, d):
        return remote(4, c, d, held['fbuf'].at[lax.rem(c, 2), at(far * quarter + d * q_half, q_half, q_half), :], r1.at[lax.rem(c, 2), d])

    def r_second(c, d):
        return remote(5, c, d, held['fbuf'].at[lax.rem(c, 2), at((right, left)[d] * quarter, quarter, quarter), :], r2.at[lax.rem(c, 2), d])

    def o_half(kind, c, d, part):
        rows_of = c * rows + me * quarter + part * q_half
        return remote(kind, c, d, out_q.at[c, pl.ds(part * q_half, q_half), :], out.at[at(rows_of, q_half, q_half), :])

    def o_first(c, d):
        return o_half(6, c, d, d)

    def o_other(c, d):
        return o_half(8, c, d, 1 - d)

    def o_second(c, d):
        piece = at(c * rows + (left, right)[d] * quarter + d * q_half, q_half, q_half)
        return remote(7, c, d, out.at[piece, :], out.at[piece, :])

    def start(make, c):
        make(c, 0).start()
        make(c, 1).start()

    def arrived(make, c):
        make(c, 0).wait_recv()
        make(c, 1).wait_recv()

    def sent(make, c):
        make(c, 0).wait_send()
        make(c, 1).wait_send()

    share = w_out.shape[0] // 2
    core = lax.rem(my_e, 2)
    core_rows = at(core * share, share, share)

    def w_first(k):
        peer = lax.rem(me + k, tp)
        return pltpu.make_async_remote_copy(
            src_ref=w_out.at[core_rows, at(peer * width, width, width)], dst_ref=wx.at[me, core_rows, :],
            send_sem=wsend.at[0, k], recv_sem=wrecv.at[0, k], device_id={'tp': peer}, device_id_type=MESH)

    def w_second(k):
        piece = wx.at[lax.rem(me + tp - k, tp), core_rows, :]
        return pltpu.make_async_remote_copy(
            src_ref=piece, dst_ref=piece, send_sem=wsend.at[1, k], recv_sem=wrecv.at[1, k],
            device_id={'ep': my_e + 1 - 2 * core}, device_id_type=MESH)

    def w_start():
        for k in range(1, tp):
            w_first(k).start()

    def w_pair():
        for k in range(1, tp):
            w_first(k).wait_recv()
            w_second(k).start()

    def w_done():
        for k in range(1, tp):
            w_second(k).wait_recv()

    def w_sent():
        for k in range(1, tp):
            w_first(k).wait_send()
            w_second(k).wait_send()

    class Pair:
        def __init__(self, wa, wb):
            self.refs = (wa, wb)
            self.full, self.tail = wa.shape[0] // TILE, wa.shape[0] % TILE
            self.tiles = self.full + (self.tail > 0)

        def copies(self, i, slot, n=TILE):
            return [pltpu.make_async_copy(w.at[at(i * TILE, n, 32), :], wb1.at[slot, k, pl.ds(0, n), :], sem1.at[slot, k]) for k, w in enumerate(self.refs)]

        def go(self, i, slot, n=TILE):
            for cp in self.copies(i, slot, n):
                cp.start()

        def ready(self, i, slot, n=TILE):
            for cp in self.copies(i, slot, n):
                cp.wait()

    nt_ahead = NT_SLOTS - 1

    def gate_up(lhs, h, pair, base, then, mid=None):
        full, tail = pair.full, pair.tail

        def product(slot, n):
            dims = (((1,), (1,)), ((), ()))
            gate = lax.dot_general(lhs[:h.shape[0], :], wb1[slot, 0, :n, :], dims, preferred_element_type=F32)
            up = lax.dot_general(lhs[:h.shape[0], :], wb1[slot, 1, :n, :], dims, preferred_element_type=F32)
            return (jax.nn.silu(gate) * up).astype(BF16)

        def step(i, carry):
            nxt = i + nt_ahead
            ahead = lax.rem(base + nxt, NT_SLOTS)
            pl.when(nxt < full)(lambda: pair.go(nxt, ahead))
            if tail:
                pl.when(nxt == full)(lambda: pair.go(full, ahead, tail))
            pl.when(nxt >= pair.tiles)(lambda: then(nxt - pair.tiles, ahead))
            slot = lax.rem(base + i, NT_SLOTS)
            pair.ready(i, slot)
            h[:, at(i * TILE, TILE, TILE)] = product(slot, TILE)
            if mid is not None:
                pl.when(i == full // 2)(mid)
            return carry

        lax.fori_loop(0, full, step, 0)
        if tail:
            then(full + nt_ahead - pair.tiles, lax.rem(base + full + nt_ahead, NT_SLOTS))
            slot = lax.rem(base + full, NT_SLOTS)
            pair.ready(full, slot, tail)
            h[:, full * TILE:full * TILE + tail] = product(slot, tail)

    nn_ahead = NN_SLOTS - 1

    def go(fetch, i, slot):
        for cp in fetch(i, slot):
            cp.start()

    def prime(fetch):
        for j in range(nn_ahead):
            go(fetch, j, j)

    def columns(left_ref, m, depth, tiles, fetch, use, then=None, off=0):
        def step(i, carry):
            nxt = i + nn_ahead
            ahead = lax.rem(nxt, NN_SLOTS)
            pl.when(nxt < tiles)(lambda: go(fetch, nxt, ahead))
            if then is not None:
                pl.when(nxt >= tiles)(lambda: then(nxt - tiles, ahead))
            slot = lax.rem(i, NN_SLOTS)
            for cp in fetch(i, slot):
                cp.wait()
            use(i, slot, jnp.dot(left_ref[off:off + m, :depth], wb2[slot, :depth, :], preferred_element_type=F32))
            return carry

        lax.fori_loop(0, tiles, step, 0)

    def whole_depth(w):
        def fetch(i, slot):
            return [pltpu.make_async_copy(w.at[:, at(i * TILE, TILE, TILE)], wb2.at[slot, pl.ds(0, w.shape[0]), :], sem2.at[slot, 0])]
        return fetch

    experts_in = Pair(eg, eu)
    ffn_in = Pair(wg, wu)
    from_qkv, from_ed, from_wd = whole_depth(wqkv), whole_depth(ed), whole_depth(wd)

    def from_out(i, slot):
        cols = at(i * TILE, TILE, TILE)
        own = pltpu.make_async_copy(w_out.at[:, at(me * width + i * TILE, TILE, TILE)], wb2.at[slot, at(me * width, width, width), :], sem2.at[slot, 0])
        rest = [pltpu.make_async_copy(wx.at[who, :, cols], wb2.at[slot, at(who * width, width, width), :], sem2.at[slot, k])
                for k, who in ((1, right), (2, far), (3, left))]
        return [own] + rest

    pair_rows = seq // PAIRS
    e_rows = slots_all // E_BLOCKS

    def c_forward(c):
        arrived(c_first, c)
        start(c_second, c)

    chips = ep // 2
    my_chip = my_e // 2
    order = sorted(((m, flip) for m in range(chips) for flip in range(2)), key=lambda v: (-min(v[0], chips - v[0]), -v[1]))
    place = {v: q for q, v in enumerate(order)}
    others = range(ep - 1)

    def peer_of(q):
        m, flip = order[q]
        return 2 * lax.rem(my_chip + m, chips) + (1 - core if flip else core)

    def back_place(q):
        m, flip = order[q]
        return place[((chips - m) % chips, flip)]

    def d_copy(q):
        peer = peer_of(q)
        return pltpu.make_async_remote_copy(
            src_ref=send.at[at(peer * sub, sub, sub), :], dst_ref=recv.at[pl.ds(back_place(q) * sub, sub), :],
            send_sem=dsend.at[q], recv_sem=drecv.at[q], device_id={'ep': peer}, device_id_type=MESH)

    own_rows = at(my_e * sub, sub, sub)

    def y_copy(q):
        return pltpu.make_async_remote_copy(
            src_ref=y.at[pl.ds(q * sub, sub), :], dst_ref=back.at[own_rows, :],
            send_sem=ysend.at[q], recv_sem=yrecv.at[q], device_id={'ep': peer_of(q)}, device_id_type=MESH)


    def y_back():
        for q in others:
            y_copy(q).wait_recv()

    def a_forward(c):
        arrived(a_first, c)
        start(a_second, c)

    w_start()
    lanes = gain_flat.shape[1]
    per = d_model // lanes
    for k in range(gain_flat.shape[0]):
        gain[k // per:k // per + 1, (k % per) * lanes:(k % per + 1) * lanes] = gain_flat[k:k + 1, :]

    def prepare(u, pick, x_in, n_out, piled):
        size = x_in.shape[1]
        blocks = seq // size

        def x_get(i, k):
            return pltpu.make_async_copy(x.at[at(i * size, size, size), :], x_in.at[k], sem2.at[k, 0])

        def n_put(i, k):
            return pltpu.make_async_copy(n_out.at[k], n.at[at(i * size, size, size), :], sem3.at[k])

        x_get(0, 0).start()

        def norm(i, carry):
            k = lax.rem(i, 2)
            pl.when(i + 1 < blocks)(lambda: x_get(i + 1, 1 - k).start())
            pl.when(i >= 2)(lambda: n_put(i - 2, k).wait())
            x_get(i, k).wait()
            mine = at(i * size, size, size)
            val = x_in[k].astype(F32)
            unit = val * lax.rsqrt(jnp.mean(val * val, axis=-1, keepdims=True) + EPS)
            n_out[k] = (unit * gain[0:1, :]).astype(BF16)
            n_put(i, k).start()
            row = (unit * gain[1:2, :]).astype(BF16)
            u[mine, :] = row
            logits = lax.dot_general(wr[...], row, (((1,), (1,)), ((), ())), preferred_element_type=F32)
            expert = lax.broadcasted_iota(jnp.int32, logits.shape, 0)
            picked = [jnp.sum(jnp.where(expert == ids[j:j + 1, mine], logits, 0.0), axis=0, keepdims=True) for j in range(top_k)]
            top = functools.reduce(jnp.maximum, picked)
            weights = [jnp.exp(p - top) for p in picked]
            total = sum(weights)
            for j in range(top_k):
                route[top_k + j:top_k + j + 1, mine] = weights[j] / total
            return carry
        lax.fori_loop(0, blocks, norm, 0)
        rows_all = lax.broadcasted_iota(jnp.int32, pick.shape, 0)
        hit = None
        for j in range(top_k):
            slot = slots[j:j + 1, :]
            row_of = jnp.where(lax.rem(slot, tp) == me, ids[j:j + 1, :] * sub + lax.div(slot, tp), -1)
            route[j:j + 1, :] = row_of.astype(F32)
            match = rows_all == row_of
            hit = match if hit is None else hit | match
        pick[...] = jnp.where(hit, 1.0, 0.0).astype(BF16)
        cols = piled.shape[2]
        parts = d_model // cols

        def put(i, k):
            return pltpu.make_async_copy(piled.at[k], send.at[:, at(i * cols, cols, cols)], sem1.at[k, 0])

        def gather(i, carry):
            k = lax.rem(i, 2)
            pl.when(i >= 2)(lambda: put(i - 2, k).wait())
            piled[k] = jnp.dot(pick[...], u[:, at(i * cols, cols, cols)], preferred_element_type=F32).astype(BF16)
            put(i, k).start()
            return carry
        lax.fori_loop(0, parts, gather, 0)
        for i in range(parts - 2, parts):
            put(i, i % 2).wait()
        for i in range(blocks - 2, blocks):
            n_put(i, i % 2).wait()

    tokens = 256
    pl.run_scoped(
        prepare, pltpu.VMEM((seq, d_model), BF16), pltpu.VMEM((slots_all, seq), BF16), pltpu.VMEM((2, tokens, d_model), BF16),
        pltpu.VMEM((2, tokens, d_model), BF16), pltpu.VMEM((2, slots_all, 1024), BF16))
    for q in others:
        d_copy(q).start()

    head_dim = width // heads
    low = head_dim // 2

    def first_half(lhs, he, qkv, ystage, acc):
        held['qkv'] = qkv

        def n_load(p):
            return pltpu.make_async_copy(n.at[pl.ds(p * pair_rows, pair_rows), :], lhs.at[pl.ds(0, pair_rows), :], lsem.at[0])

        def rotate(val, piece):
            parts = []
            for k in range(TILE // head_dim):
                one = val[:, k * head_dim:(k + 1) * head_dim]
                parts.append(one * cos_ref[piece, :] + pltpu.roll(one, low, 1) * sin_ref[piece, :])
            return jnp.concatenate(parts, axis=1)

        def settle(piece, i, val):
            val = jnp.where(i < 2 * width // TILE, rotate(val, piece), val)
            qkv[piece, at(i * TILE, TILE, TILE)] = val.astype(BF16)

        def project_in(start_row, count, off, follow, between=None):
            piece = pl.ds(start_row, count)

            def keep(i, slot, val):
                settle(piece, i, val)

            def then(i, slot):
                if between is not None:
                    pl.when(i == 0)(between)
                go(follow, i, slot)
            columns(lhs, count, d_model, 3 * width // TILE, from_qkv, keep, then, off)

        def attend(c):
            base = c * rows
            keys = base + rows
            dims = (((1,), (1,)), ((), ()))

            def two(g, carry):
                for k in range(2):
                    hh = 2 * g + k
                    lane = lambda off: at(off + hh * head_dim, head_dim, head_dim)
                    query = qkv[base:keys, lane(0)]
                    scores = lax.dot_general(query, qkv[base:keys, lane(width)], dims, preferred_element_type=F32)
                    row = lax.broadcasted_iota(jnp.int32, scores.shape, 0)
                    col = lax.broadcasted_iota(jnp.int32, scores.shape, 1)
                    scores = jnp.where(row >= col, scores, -1e30)
                    if c:
                        before = lax.dot_general(query, qkv[0:base, lane(width)], dims, preferred_element_type=F32)
                        scores = jnp.concatenate([before, scores], axis=1)
                    top = jnp.max(scores, axis=1, keepdims=True)
                    prob = jnp.exp2((scores - top) * (head_dim ** -0.5 * LOG2E))
                    prob = (prob * (1.0 / jnp.sum(prob, axis=1, keepdims=True))).astype(BF16)
                    qkv[base:keys, lane(0)] = jnp.dot(prob, qkv[0:keys, lane(2 * width)], preferred_element_type=F32).astype(BF16)
                return carry
            lax.fori_loop(0, heads // 2, two, 0)

        def x_load(b):
            far = e_rows - (sub if b == E_BLOCKS - 1 else 0)
            copies = [pltpu.make_async_copy(recv.at[pl.ds(b * e_rows, far), :], lhs.at[pl.ds(0, far), :], lsem.at[0])]
            if far < e_rows:
                copies.append(pltpu.make_async_copy(send.at[own_rows, :], lhs.at[pl.ds(far, sub), :], lsem.at[1]))
            return copies

        def expert(b, mid):
            loads = x_load(b)
            for cp in loads:
                cp.start()
            for cp in loads:
                cp.wait()
            last = b == E_BLOCKS - 1
            gate_up(lhs, he, experts_in, b * experts_in.tiles, ffn_in.go if last else experts_in.go, mid)
            tiles = d_model // TILE

            far = e_rows - (sub if last else 0)

            def puts(i):
                k = lax.rem(i, 2)
                cols = at(i * TILE, TILE, TILE)
                copies = [pltpu.make_async_copy(ystage.at[k, pl.ds(0, far), :], y.at[pl.ds(b * e_rows, far), cols], ysem.at[k, 0])]
                if last:
                    copies.append(pltpu.make_async_copy(ystage.at[k, pl.ds(far, sub), :], back.at[own_rows, cols], ysem.at[k, 1]))
                return copies

            def put(i):
                for cp in puts(i):
                    cp.start()

            def put_wait(i):
                for cp in puts(i):
                    cp.wait()

            def keep(i, slot, acc):
                pl.when(i >= 2)(lambda: put_wait(i - 2))
                ystage[lax.rem(i, 2)] = acc.astype(BF16)
                put(i)
            follow = from_out if last else from_ed
            columns(he, e_rows, ed.shape[0], tiles, from_ed, keep, lambda i, slot: go(follow, i, slot))
            put_wait(tiles - 2)
            put_wait(tiles - 1)
            span = ep // E_BLOCKS
            for k in range(b * span, (b + 1) * span):
                if k < ep - 1:
                    y_copy(k).start()

        def project_out(p):
            for k in range(CHUNKS // PAIRS):
                arrived(c_second, p * (CHUNKS // PAIRS) + k)
            piece = pl.ds(p * pair_rows, pair_rows)
            here = pl.ds(0, pair_rows)
            loads = [pltpu.make_async_copy(src.at[piece, :], lhs.at[here, at(who * width, width, width)], lsem.at[k])
                     for k, (src, who) in enumerate(((c_r, right), (c_o, far), (c_l, left)))]
            loads.append(pltpu.make_async_copy(x.at[piece, at(me * width, width, width)], a_own.at[piece, :], lsem.at[4]))
            for cp in loads:
                cp.start()
            lhs[here, at(me * width, width, width)] = qkv[piece, 0:width]
            for cp in loads:
                cp.wait()

            def keep(i, slot, acc):
                block = (piece, at(i * TILE, TILE, TILE))
                a_own[block] = (a_own[block].astype(F32) + acc).astype(BF16)
            follow = from_ed if p < PAIRS - 1 else from_wd
            columns(lhs, pair_rows, d_model, width // TILE, from_out, keep, lambda i, slot: go(follow, i, slot))

        second_load = pltpu.make_async_copy(n.at[pl.ds(rows, rows), :], lhs.at[pl.ds(rows, rows), :], lsem.at[0])
        second_load.start()
        acc[...] = jnp.zeros_like(acc)
        depth_block = 256
        pltpu.emit_pipeline(
            functools.partial(relay_kernel, heads, acc),
            grid=(d_model // depth_block,),
            in_specs=[pl.BlockSpec((rows, depth_block), lambda i: (0, i), pipeline_mode=pl.Buffered(3))]
            + [pl.BlockSpec((depth_block * heads, head_dim), lambda i: (i, 0), pipeline_mode=pl.Buffered(3))] * 3,
            out_specs=[pl.BlockSpec((depth_block, 3 * width), lambda i: (i, 0))],
        )(n, wq, wk, wv, wqkv)
        prime(from_qkv)

        def settle_first(i, carry):
            settle(pl.ds(0, rows), i, acc[:, at(i * TILE, TILE, TILE)])
            return carry
        lax.fori_loop(0, 3 * width // TILE, settle_first, 0)
        attend(0)
        start(c_first, 0)
        second_load.wait()
        project_in(rows, rows, rows, from_qkv)
        n_load(1).start()
        attend(1)
        start(c_first, 1)
        for k in range(nt_ahead):
            experts_in.go(k, k)
        w_pair()
        n_load(1).wait()
        c_forward(0)
        project_in(2 * rows, 2 * rows, 0, from_out, w_done)
        c_forward(1)
        attend(2)
        start(c_first, 2)
        attend(3)
        start(c_first, 3)
        project_out(0)
        start(a_first, 0)
        for q in others:
            d_copy(q).wait_recv()
        expert(0, lambda: c_forward(2))
        c_forward(3)

        def late():
            a_forward(0)
            start(a_first, 1)
        expert(1, late)
        project_out(1)
        for c in range(CHUNKS):
            sent(c_first, c)

    pl.run_scoped(
        first_half, pltpu.VMEM((max(pair_rows, e_rows), d_model), BF16), pltpu.VMEM((e_rows, ed.shape[0]), BF16),
        pltpu.VMEM((seq, 3 * width), BF16), pltpu.VMEM((2, e_rows, TILE), BF16),
        pltpu.VMEM((rows, 3 * width), F32))
    start(a_first, 2)

    def second_half(lhs, h, fbuf, a_in, sel, gates):
        held['fbuf'] = fbuf

        def reduce_on(c):
            for d, who in ((0, right), (1, left)):
                r_first(c, d).wait_recv()

                def add(k, carry, d=d, who=who):
                    block = (lax.rem(c, 2), at(who * quarter + d * q_half + k * 8, 8, 8), slice(None))
                    fbuf[block] = fbuf[block] + r1[lax.rem(c, 2), d, at(k * 8, 8, 8), :]
                    return carry
                lax.fori_loop(0, q_half // 8, add, 0)
            start(r_second, c)

        def o_local(c):
            return pltpu.make_async_copy(out_q.at[c], out.at[at(c * rows + me * quarter, quarter, quarter), :], osem.at[c])

        def finish(c):
            arrived(r_second, c)

            def add(k, carry):
                part = at(k * 16, 16, 16)
                total = fbuf[lax.rem(c, 2), at(me * quarter + k * 16, 16, 16), :] + (r2[lax.rem(c, 2), 0, part, :] + r2[lax.rem(c, 2), 1, part, :])
                out_q[c, part, :] = (a_mine[c, part, :].astype(F32) + total).astype(BF16)
                return carry
            lax.fori_loop(0, quarter // 16, add, 0)
            start(o_first, c)
            start(o_other, c)
            o_local(c).start()

        def o_forward(c):
            arrived(o_first, c)
            start(o_second, c)

        def from_back(i, slot):
            return pltpu.make_async_copy(back.at[:, at(i * TILE, TILE, TILE)], wb3.at[slot], sem3.at[slot])

        def copies_prime():
            for k in range(nn_ahead):
                from_back(k, k).start()

        def combine(c):
            tiles = d_model // TILE

            def step(i, carry):
                nxt = i + nn_ahead
                pl.when(nxt < tiles)(lambda: from_back(nxt, lax.rem(nxt, NN_SLOTS)).start())
                slot = lax.rem(i, NN_SLOTS)
                from_back(i, slot).wait()
                copies = jnp.dot(sel[...], wb3[slot], preferred_element_type=F32)
                block = (lax.rem(c, 2), slice(None), at(i * TILE, TILE, TILE))
                total = fbuf[block]
                for j in range(top_k):
                    total = total + gates[:, j:j + 1] * copies[j * rows:(j + 1) * rows]
                fbuf[block] = total
                return carry
            lax.fori_loop(0, tiles, step, 0)

        def ffn(c, carry):
            arrived(a_second, c)
            piece = at(c * rows, rows, rows)
            loads = [pltpu.make_async_copy(src.at[piece, :], a_in.at[k], lsem.at[k]) for k, src in enumerate((a_r, a_o, a_l))]
            for cp in loads:
                cp.start()
            for cp in loads:
                cp.wait()
            parts = ((None, me), (0, right), (1, far), (2, left))

            def norm(k, carry):
                block = at(k * 16, 16, 16)
                vals = [(a_own[at(c * rows + k * 16, 16, 16), :] if p is None else a_in[p, block, :]).astype(F32) for p, _ in parts]
                square = sum(jnp.sum(v * v, axis=1, keepdims=True) for v in vals)
                inv = lax.rsqrt(square / d_model + EPS)
                for v, (_, who) in zip(vals, parts):
                    cols = at(who * width, width, width)
                    lhs[block, cols] = (v * inv * gain[2:3, cols]).astype(BF16)
                return carry
            lax.fori_loop(0, rows // 16, norm, 0)
            for p, who in parts:
                mine = at(me * quarter, quarter, quarter)
                val = a_own[at(c * rows + me * quarter, quarter, quarter), :] if p is None else a_in[p, mine, :]
                a_mine[c, :, at(who * width, width, width)] = val
            table = jnp.transpose(route[:, piece])
            lane = lax.broadcasted_iota(jnp.int32, (rows, slots_all), 1).astype(F32)
            for j in range(top_k):
                sel[j * rows:(j + 1) * rows, :] = jnp.where(lane == table[:, j:j + 1], 1.0, 0.0).astype(BF16)
                gates[:, j:j + 1] = table[:, top_k + j:top_k + j + 1]

            def mid():
                @pl.when(c == 0)
                def _():
                    a_forward(1)
                    start(a_first, 3)
                pl.when(c >= 1)(lambda: reduce_on(c - 1))
            def after(i, slot):
                pl.when(c < CHUNKS - 1)(lambda: ffn_in.go(i, slot))
            gate_up(lhs, h, ffn_in, E_BLOCKS * experts_in.tiles + c * ffn_in.tiles, after, mid)
            pl.when(c == 0)(lambda: a_forward(2))

            @pl.when(c >= 2)
            def _():
                o_forward(c - 2)
                sent(r_first, c - 2)
                sent(r_second, c - 2)

            def keep(i, slot, acc):
                fbuf[lax.rem(c, 2), :, at(i * TILE, TILE, TILE)] = acc

            def then(i, slot):
                pl.when(c < CHUNKS - 1)(lambda: go(from_wd, i, slot))
            pl.when(c > 0)(copies_prime)
            columns(h, rows, wd.shape[0], d_model // TILE, from_wd, keep, then)

            @pl.when(c == 0)
            def _():
                a_forward(3)
                y_back()
                copies_prime()
            combine(c)
            start(r_first, c)
            pl.when(c >= 1)(lambda: finish(c - 1))
            return carry
        lax.fori_loop(0, CHUNKS, ffn, 0)
        reduce_on(CHUNKS - 1)
        o_forward(CHUNKS - 2)
        finish(CHUNKS - 1)
        o_forward(CHUNKS - 1)

        def drain(c, carry):
            arrived(o_second, c)
            arrived(o_other, c)
            o_local(c).wait()
            for make in (c_second, a_first, a_second, o_first, o_other, o_second):
                sent(make, c)

            @pl.when(c >= CHUNKS - 2)
            def _():
                sent(r_first, c)
                sent(r_second, c)
            return carry
        lax.fori_loop(0, CHUNKS, drain, 0)
        for q in others:
            d_copy(q).wait_send()
            y_copy(q).wait_send()
        w_sent()

    pl.run_scoped(
        second_half, pltpu.VMEM((rows, d_model), BF16), pltpu.VMEM((rows, wd.shape[0]), BF16), pltpu.VMEM((2, rows, d_model), F32),
        pltpu.VMEM((3, rows, width), BF16), pltpu.VMEM((top_k * rows, slots_all), BF16), pltpu.VMEM((rows, top_k), F32))


def fused_layer(tp, ep, heads, slots_all, wq, wk, wv, w_out, x, gains, wg, wu, wd, eg, eu, ed, router, ids, slots, cos, sin):
    seq, d_model = x.shape
    rows = seq // CHUNKS
    quarter = rows // tp
    width = d_model // tp
    hidden = wd.shape[0]
    any_spec = pl.BlockSpec(memory_space=pl.ANY)
    vmem_spec = pl.BlockSpec(memory_space=pltpu.VMEM)
    part = jax.ShapeDtypeStruct((seq, width), BF16)
    copies = jax.ShapeDtypeStruct((slots_all, d_model), BF16)
    outs = pl.pallas_call(
        functools.partial(layer_kernel, tp, ep, heads),
        out_shape=[jax.ShapeDtypeStruct((seq, d_model), BF16)] * 2 + [copies, jax.ShapeDtypeStruct((d_model, 3 * width), BF16)] + [part] * 6
        + [jax.ShapeDtypeStruct((tp, w_out.shape[0], width), BF16)] + [copies] * 3,
        in_specs=[any_spec] * 5 + [vmem_spec] + [any_spec] * 6 + [vmem_spec] * 5,
        out_specs=[any_spec] * 14,
        scratch_shapes=[
            pltpu.VMEM((3, d_model), F32),
            pltpu.VMEM((8, seq), F32),
            pltpu.VMEM((2, 2, quarter // 2, d_model), F32),
            pltpu.VMEM((2, 2, quarter, d_model), F32),
            pltpu.VMEM((seq, width), BF16),
            pltpu.VMEM((CHUNKS, quarter, d_model), BF16),
            pltpu.VMEM((CHUNKS, quarter, d_model), BF16),
            pltpu.VMEM((NT_SLOTS, 2, TILE, d_model), BF16),
            pltpu.VMEM((NN_SLOTS, d_model, TILE), BF16),
            pltpu.VMEM((NN_SLOTS, slots_all, TILE), BF16),
            pltpu.SemaphoreType.DMA((9, CHUNKS, 2)),
            pltpu.SemaphoreType.DMA((9, CHUNKS, 2)),
            pltpu.SemaphoreType.DMA((ep,)),
            pltpu.SemaphoreType.DMA((ep,)),
            pltpu.SemaphoreType.DMA((ep,)),
            pltpu.SemaphoreType.DMA((ep,)),
            pltpu.SemaphoreType.DMA((2, 2)),
            pltpu.SemaphoreType.DMA((2, tp)),
            pltpu.SemaphoreType.DMA((2, tp)),
            pltpu.SemaphoreType.DMA((NT_SLOTS, 2)),
            pltpu.SemaphoreType.DMA((NN_SLOTS, 4)),
            pltpu.SemaphoreType.DMA((NN_SLOTS,)),
            pltpu.SemaphoreType.DMA((5,)),
            pltpu.SemaphoreType.DMA((CHUNKS,)),
        ],
        compiler_params=pltpu.CompilerParams(collective_id=0, has_side_effects=True, vmem_limit_bytes=67043328),
        cost_estimate=pl.CostEstimate(flops=6 * seq * d_model * hidden, bytes_accessed=300 * 2 ** 20, transcendentals=seq * hidden),
    )(wq, wk, wv, w_out, x, gains, wg, wu, wd, eg, eu, ed, router, ids, slots, cos, sin)
    return outs[0]


def solution(mesh):
    tok_spec = P(('dp', 'ep'), None, None)
    col_spec = P(None, 'tp', None)
    exp_spec = P('ep', None, None)
    in_specs = (tok_spec, tok_spec, tok_spec, P(None), col_spec, col_spec, col_spec, P('tp', None, None), P(None), P(None, 'tp'), P(None, 'tp'), P('tp', None), P(None), P(None, None), exp_spec, exp_spec, exp_spec)
    tp = mesh.shape['tp']
    ep = mesh.shape['ep']

    def layer_local(hidden_in, expert_ids, slot_ids, attn_gain, w_query, w_key, w_value, w_out, ffn_gain, w_gate, w_up, w_down, moe_gain, w_router, exp_gate, exp_up, exp_down):
        _, seq, d_model = hidden_in.shape
        heads, head_dim = w_query.shape[1:]
        experts = w_router.shape[1]
        top_k = expert_ids.shape[2]
        cap = 3 * seq * top_k // (2 * experts)
        sub = cap // tp
        x = hidden_in[0]
        gains = jnp.concatenate([attn_gain, moe_gain, ffn_gain]).astype(F32).reshape(-1, 128)
        cos, sin = rope_tables(seq, head_dim)
        flat = lambda w: w.reshape(d_model * heads, head_dim)
        out = fused_layer(tp, ep, heads, experts * sub, flat(w_query), flat(w_key), flat(w_value), w_out.reshape(heads * head_dim, d_model), x,
                          gains, w_gate.T, w_up.T, w_down, exp_gate[0].T, exp_up[0].T, exp_down[0],
                          w_router.T, expert_ids[0].T, slot_ids[0].T, cos, sin)
        return out[None]

    return jax.shard_map(layer_local, mesh=mesh, in_specs=in_specs, out_specs=tok_spec, check_vma=False)
```
